128 devices in a mesh: section: 8 (over x, core), ep: 16 (over y, z).
Axes of the slice: x: 4, y: 4, z: 4, core: 2. Of those that a mesh axis runs over, the one named last changes fastest.
Arguments:
- output_grad: bfloat16 [8, 4096, 1024], P('section', 'ep'), may hold values from -6 to 6
- layer_input: bfloat16 [8, 4096, 1024], P('section', 'ep'), may hold values from -6 to 6
- expert_ids: int32 [8, 4096, 8], P('section', 'ep'), may hold values from 0 to 63, all different within a row; in each aligned block of 256 rows (0 to 255, 256 to 511, ..., all dimensions but the last counted through in order) at most 40 rows name the same one
- route_probs: bfloat16 [8, 4096, 8], P('section', 'ep'), may hold values from 0.049804688 to 0.44921875
- gate_weight: bfloat16 [8, 64, 1024, 384], P('section', 'ep'), may hold values from -0.1875 to 0.1875
- up_weight: bfloat16 [8, 64, 1024, 384], P('section', 'ep'), may hold values from -0.1875 to 0.1875
- down_weight: bfloat16 [8, 64, 384, 1024], P('section', 'ep'), may hold values from -0.3125 to 0.3125
- saved_inputs: bfloat16 [8, 64, 640, 1024], P('section', 'ep'), may hold values from -6 to 6
- saved_gate_grad: bfloat16 [8, 64, 640, 384], P('section', 'ep'), may hold values from -0.5 to 0.5
- saved_up_grad: bfloat16 [8, 64, 640, 384], P('section', 'ep'), may hold values from -0.5 to 0.5
- saved_counts: int32 [8, 64, 16], P('section', 'ep'), may hold values from 0 to 40, as said below
Outputs:
- upstream_grad: bfloat16 [8, 4096, 1024], P('section', 'ep')
- prob_grad: bfloat16 [8, 4096, 8], P('section', 'ep')
- gate_weight_grad: bfloat16 [8, 64, 1024, 384], P('section', 'ep')
- up_weight_grad: bfloat16 [8, 64, 1024, 384], P('section', 'ep')
The draws below stay inside these ranges and needn't reach their ends.
Inputs may be any that keep to these rules, and one draw needn't show every extreme that they name: `expert_ids`: each token names 8 different experts. Among the tokens of one device (aligned blocks of 256 tokens of a section) no expert is named more than 40 times, a bound that some block reaches. `saved_counts`: rows of a block at or beyond its count are padding; some block is full in every draw.
All inputs are finite; a program needn't handle non-finite values.
Results may differ from the reference program's by a relative error of at most 0.008.
Values may be sent and summed in bfloat16 or wider, within the bound.
A program may use at most 128 MiB of HBM per device.

```python
import math
import jax
import jax.numpy as jnp
import numpy as np
from jax import lax

D = 1024
FF = 384
TOP = 8
TOK_DEV = 256
SECTIONS = 8
TOKENS = 4096
EXPERTS = 64
SOURCES = 16
CAP = 40
SLOTS = 640
N_EP = 16


def draw_saved_counts(key, part):
    base = jax.random.randint(jax.random.fold_in(key, 11), (SECTIONS, EXPERTS, SOURCES), 0, CAP + 1)
    chosen = jax.random.randint(jax.random.fold_in(key, 12), (SECTIONS, 1, 1), 0, EXPERTS * SOURCES)
    flat = jnp.arange(EXPERTS * SOURCES, dtype=jnp.int32).reshape(1, EXPERTS, SOURCES)
    return jnp.where(flat == chosen, CAP, base).astype(jnp.int32)


def block_scale(rng, shape, shards, least, high):
    factor_of, own = 1.0, jax.random.fold_in(rng, 6)
    for axis_at, blocks in shards:
        draws = jnp.exp(jax.random.uniform(jax.random.fold_in(own, axis_at), (blocks,), jnp.float32, least / len(shards), high / len(shards)))
        factor_of = factor_of * jnp.repeat(draws, shape[axis_at] // blocks).reshape([-1 if axis == axis_at else 1 for axis in range(len(shape))])
    return factor_of


def deal_out(key, own, number, rows, amount, top, reach, slope):
    sequence = jax.random.permutation(key, amount)
    packed, common = shares(amount, rows * top, reach, slope, True), shares(amount, rows * top, reach, slope, False)
    places = jnp.arange(amount)

    def named(sizes, rotation):
        used = int((sizes > 0).sum())
        fixed = max(1, used // 4)
        passed = fixed + (places - fixed + rotation * (used - fixed)) % max(1, amount - fixed)
        return jnp.zeros((amount,), jnp.int32).at[sequence[jnp.where(places < fixed, places, passed)]].set(jnp.asarray(sizes, jnp.int32))

    sizes = jnp.where(number % 4 == 0, named(packed, number // 4), named(common, number - number // 4 - 1))
    mixed = jax.random.permutation(jax.random.fold_in(own, 3), amount)
    giver, receiver = mixed[0:amount // 2 * 2:2], mixed[1:amount // 2 * 2:2]
    slack = jnp.minimum(sizes[giver] - 1, reach - sizes[receiver]) // 2
    slack = jnp.where((giver == sequence[0]) | (receiver == sequence[0]) | (sizes[receiver] == 0), 0, jnp.maximum(slack, 0))
    passed = jax.random.randint(jax.random.fold_in(own, 4), (amount // 2,), 0, 1 << 20) % (slack + 1)
    sizes = sizes.at[giver].add(-passed).at[receiver].add(passed)
    labels = jnp.searchsorted(jnp.cumsum(sizes), jnp.arange(rows * top), side="right").astype(jnp.int32)
    grid = labels.reshape(top, rows).T
    grid = grid[jax.random.permutation(jax.random.fold_in(own, 1), rows)]
    rotation = jax.random.randint(jax.random.fold_in(own, 2), (rows, 1), 0, top)
    return jnp.take_along_axis(grid, (jnp.arange(top)[None, :] + rotation) % top, axis=1)


def shares(amount, total, limit, skew, full):
    weights = [(1 << 20) // math.isqrt(rank ** skew) + 1 for rank in range(1, amount + 1)]
    largest = limit if full else min(limit, max(-(-total // amount), total * weights[0] // sum(weights)))
    least = 1 if total - largest >= amount - 1 else 0
    given, spare = [largest] + [least] * (amount - 1), total - largest - least * (amount - 1)
    while spare > 0:
        free = [i for i in range(1, amount) if given[i] < largest] or [i for i in range(1, amount) if given[i] < limit]
        whole, budget = sum([weights[i] for i in free]), spare
        for i in free:
            more = min(limit - given[i], max(1, budget * weights[i] // whole), spare)
            given[i] = given[i] + more
            spare = spare - more
    return np.array(given)


def scatter_about(key, shape, deviation, reach, pieces=(), held_as=jnp.bfloat16):
    values = jax.random.normal(key, shape, jnp.float32) * deviation
    if len(pieces) > 0:
        values = block_scale(key, shape, pieces, -0.22, 0.18) * values
    return jnp.clip(values, min=-reach, max=reach).astype(held_as)


def setup_inputs(seed: int = 0) -> dict:
    splits = jax.random.split(jax.random.key(seed), 12)
    output_grad = scatter_about(splits[0], (SECTIONS, TOKENS, D), 1.0, 6.0, ((0, 8), (1, 16)))
    layer_input = scatter_about(splits[1], (SECTIONS, TOKENS, D), 1.0, 6.0, ((0, 8), (1, 16)))
    expert_ids_keys = jax.random.split(jax.random.fold_in(splits[2], 1), SECTIONS * TOKENS // TOK_DEV)
    expert_ids_turns = jax.random.permutation(jax.random.fold_in(splits[2], 3), SECTIONS * TOKENS // TOK_DEV)
    expert_ids = jax.vmap(lambda own, number: deal_out(jax.random.fold_in(splits[2], 2), own, number, TOK_DEV, EXPERTS, TOP, CAP, 2))(expert_ids_keys, expert_ids_turns).reshape((SECTIONS, TOKENS, TOP))
    route_probs = jnp.clip(0.049804688 + 0.39941406 * jax.random.uniform(splits[3], (SECTIONS, TOKENS, TOP), jnp.float32) ** block_scale(splits[3], (SECTIONS, TOKENS, TOP), ((0, 8), (1, 16)), -0.2, 0.2), 0.049804688, 0.44921875).astype(jnp.bfloat16)
    gate_weight = scatter_about(splits[4], (SECTIONS, EXPERTS, D, FF), D ** -0.5, 0.1875, ((0, 8), (1, 16)))
    up_weight = scatter_about(splits[5], (SECTIONS, EXPERTS, D, FF), D ** -0.5, 0.1875, ((0, 8), (1, 16)))
    down_weight = scatter_about(splits[6], (SECTIONS, EXPERTS, FF, D), FF ** -0.5, 0.3125, ((0, 8), (1, 16)))
    saved_inputs = scatter_about(splits[7], (SECTIONS, EXPERTS, SLOTS, D), 1.0, 6.0, ((0, 8), (1, 16)))
    saved_gate_grad = scatter_about(splits[8], (SECTIONS, EXPERTS, SLOTS, FF), 0.0625, 0.5, ((0, 8), (1, 16)))
    saved_up_grad = scatter_about(splits[9], (SECTIONS, EXPERTS, SLOTS, FF), 0.0625, 0.5, ((0, 8), (1, 16)))
    saved_counts = draw_saved_counts(jax.random.fold_in(splits[11], 71), 0)
    return {"output_grad": output_grad, "layer_input": layer_input, "expert_ids": expert_ids, "route_probs": route_probs, "gate_weight": gate_weight, "up_weight": up_weight, "down_weight": down_weight, "saved_inputs": saved_inputs, "saved_gate_grad": saved_gate_grad, "saved_up_grad": saved_up_grad, "saved_counts": saved_counts}


def block_slots(block_ids):
    flat_ids = block_ids.reshape(-1)
    onehot = (flat_ids[:, None] == jnp.arange(EXPERTS, dtype=jnp.int32)[None, :]).astype(jnp.int32)
    before = jnp.cumsum(onehot, axis=0) - onehot
    return jnp.sum(before * onehot, axis=1).astype(jnp.int32)


def expert_backward(operands):
    grad_rows, input_rows, prob_rows, w_gate, w_up, w_down = operands
    gate_pre = jnp.dot(input_rows, w_gate, preferred_element_type=jnp.float32)
    up_pre = jnp.dot(input_rows, w_up, preferred_element_type=jnp.float32)
    sigma = jax.nn.sigmoid(gate_pre)
    active = gate_pre * sigma
    hidden = (active * up_pre).astype(jnp.bfloat16)
    hidden_grad = jnp.dot(grad_rows, w_down.T, preferred_element_type=jnp.float32)
    output_rows = jnp.dot(hidden, w_down, preferred_element_type=jnp.float32)
    slot_prob = jnp.sum(output_rows * grad_rows.astype(jnp.float32), axis=1).astype(jnp.bfloat16)
    scaled = hidden_grad * prob_rows.astype(jnp.float32)[:, None]
    gate_grad = (scaled * up_pre * sigma * (1.0 + gate_pre * (1.0 - sigma))).astype(jnp.bfloat16)
    up_grad = (scaled * active).astype(jnp.bfloat16)
    slot_grad = jnp.dot(gate_grad, w_gate.T, preferred_element_type=jnp.float32)
    slot_grad = slot_grad + jnp.dot(up_grad, w_up.T, preferred_element_type=jnp.float32)
    return slot_grad.astype(jnp.bfloat16), slot_prob


def weight_pair(operands):
    masked, gate_grad, up_grad = operands
    gate_part = jnp.dot(masked.T, gate_grad, preferred_element_type=jnp.float32).astype(jnp.bfloat16)
    up_part = jnp.dot(masked.T, up_grad, preferred_element_type=jnp.float32).astype(jnp.bfloat16)
    return gate_part, up_part


def section_pass(grad, inputs, ids, probs, w_gate, w_up, w_down):
    blocks = ids.reshape(N_EP, TOK_DEV * TOP)
    slots = jax.vmap(block_slots)(blocks)
    source = jnp.arange(N_EP, dtype=jnp.int32)[:, None]
    place = (blocks * SLOTS + source * CAP + slots).reshape(-1).astype(jnp.int32)
    token = (jnp.arange(TOKENS * TOP, dtype=jnp.int32) // TOP).astype(jnp.int32)
    grad_rows = jnp.zeros((EXPERTS * SLOTS, D), jnp.bfloat16).at[place].set(grad[token])
    input_rows = jnp.zeros((EXPERTS * SLOTS, D), jnp.bfloat16).at[place].set(inputs[token])
    prob_rows = jnp.zeros((EXPERTS * SLOTS,), jnp.bfloat16).at[place].set(probs.reshape(-1))
    slot_grad, slot_prob = lax.map(expert_backward, (grad_rows.reshape(EXPERTS, SLOTS, D), input_rows.reshape(EXPERTS, SLOTS, D), prob_rows.reshape(EXPERTS, SLOTS), w_gate, w_up, w_down))
    picked = slot_grad.reshape(EXPERTS * SLOTS, D)[place]
    input_grad = jnp.sum(picked.reshape(TOKENS, TOP, D).astype(jnp.float32), axis=1).astype(jnp.bfloat16)
    prob_part = slot_prob.reshape(-1)[place].reshape(TOKENS, TOP)
    return input_grad, prob_part


def weight_pass(inputs, gate_grad, up_grad, counts):
    capacity = jnp.arange(CAP, dtype=jnp.int32)
    live = (capacity[None, None, :] < counts[:, :, None]).reshape(EXPERTS, SLOTS)
    masked = inputs * live.astype(jnp.bfloat16)[:, :, None]
    return lax.map(weight_pair, (masked, gate_grad, up_grad))


def reference(output_grad, layer_input, expert_ids, route_probs, gate_weight, up_weight, down_weight, saved_inputs, saved_gate_grad, saved_up_grad, saved_counts):
    input_grads = []
    prob_grads = []
    gate_grads = []
    up_grads = []
    for section_index in range(SECTIONS):
        input_grad, prob_part = section_pass(output_grad[section_index], layer_input[section_index], expert_ids[section_index], route_probs[section_index], gate_weight[section_index], up_weight[section_index], down_weight[section_index])
        gate_part, up_part = weight_pass(saved_inputs[section_index], saved_gate_grad[section_index], saved_up_grad[section_index], saved_counts[section_index])
        input_grads.append(input_grad)
        prob_grads.append(prob_part)
        gate_grads.append(gate_part)
        up_grads.append(up_part)
    stacked = jnp.stack(input_grads)
    upstream_grad = jnp.concatenate([stacked[1:], jnp.zeros_like(stacked[:1])], axis=0)
    return upstream_grad, jnp.stack(prob_grads), jnp.stack(gate_grads), jnp.stack(up_grads)
```

```python
import functools

import jax
import jax.numpy as jnp
from jax import lax
from jax.experimental import pallas as pl
from jax.experimental.pallas import tpu as pltpu
from jax.sharding import PartitionSpec as P

MESH = pl.DeviceIdType.MESH
BF = jnp.bfloat16
F32 = jnp.float32

BATCHES = ((0, 4, 12, 1), (3, 5, 7, 13), (15, 8, 2, 9), (6, 11, 14, 10))
DONE_IN = {i: b for b, batch in enumerate(BATCHES) for i in batch}
N_SEMS = 160


def dot(a, b):
    return jnp.dot(a, b, preferred_element_type=F32)


def dot_nt(a, b):
    return lax.dot_general(a, b, (((1,), (1,)), ((), ())), preferred_element_type=F32)


def dot_tn(a, b):
    return lax.dot_general(a, b, (((0,), (0,)), ((), ())), preferred_element_type=F32)


def kernel(
    sections, cap, pad,
    g_in, x_in, m_in, wg_in, wu_in, wd_in, si_in, sg_in, su_in, cnt,
    up_out, pg_out, go_out, uo_out,
    gbuf, xbuf, meta, wg, wu, wd,
    si, sgu_raw, sgu, gov, uov,
    slots, upper, oh, xd, gd, pv, sp,
    pa, pb, s1, fin, q, t1, gin, upv,
    ppg, ppgr, ppgt,
    ssem, rsem, lsem,
):
    T, D = gbuf.shape[1], gbuf.shape[2]
    NE, FF = wg.shape[0], wg.shape[2]
    SL = si.shape[0]
    H = T // 2
    HD = D // 2
    half = (pl.ds(0, H), pl.ds(H, H))
    sec = lax.axis_index("section")
    ep = lax.axis_index("ep")
    y, z = lax.div(ep, 4), lax.rem(ep, 4)

    def at(yy, zz):
        return {"ep": lax.rem(yy, 4) * 4 + lax.rem(zz, 4)}

    nb = {
        ("y", "R"): at(y + 1, z), ("y", "L"): at(y + 3, z),
        ("z", "R"): at(y, z + 1), ("z", "L"): at(y, z + 3),
    }
    before = {"section": lax.rem(sec + sections - 1, sections)}
    after = {"section": lax.rem(sec + 1, sections)}

    ids = {}
    sent = []

    def copy(key, src, dst, dev):
        k = ids.setdefault(key, len(ids))
        return pltpu.make_async_remote_copy(
            src_ref=src, dst_ref=dst, send_sem=ssem.at[k], recv_sem=rsem.at[k],
            device_id=dev, device_id_type=MESH,
        )

    def start(c):
        c.start()
        sent.append(c)

    def load(k, src, dst):
        return pltpu.make_async_copy(src, dst, lsem.at[k])

    own = [load(0, g_in, gbuf.at[0]), load(1, x_in, xbuf.at[0]), load(2, m_in, meta.at[0])]
    for c in own:
        c.start()
    weights = [load(3, wg_in, wg), load(4, wu_in, wu), load(5, wd_in, wd)]

    def saved(e):
        return [
            load(6, si_in.at[e], si),
            load(7, sg_in.at[e], sgu_raw.at[0]),
            load(8, su_in.at[e], sgu_raw.at[1]),
        ]

    def wout(e):
        return [load(9, gov, go_out.at[e]), load(10, uov, uo_out.at[e])]

    barrier = pltpu.get_barrier_semaphore()
    for dev in (*nb.values(), before, after):
        pl.semaphore_signal(barrier, inc=1, device_id=dev, device_id_type=MESH)
    for c in saved(0):
        c.start()
    for c in weights:
        c.start()
    pl.semaphore_wait(barrier, 6)
    for c in own:
        c.wait()

    paths = (("g", gbuf, "z", "y"), ("x", xbuf, "y", "z"))
    landing = {"R": 3, "L": 1}
    order = {"R": (0, 1), "L": (1, 0)}
    early = {"R": 0, "L": 1}

    def p1(path, way, h):
        name, buf, a, _ = path
        return copy((name, "p1", way, h), buf.at[0, half[h]], buf.at[landing[way], half[h]], nb[a, way])

    def f1(path, way):
        name, buf, a, _ = path
        h = early[way]
        return copy((name, "f1", way), buf.at[landing[way], half[h]], buf.at[2, half[h]], nb[a, way])

    def p2(path, way, d, h):
        name, buf, _, b = path
        return copy(
            (name, "p2", way, d, h), buf.at[d, half[h]],
            buf.at[landing[way] * 4 + d, half[h]], nb[b, way],
        )

    def f2(path, way, d):
        name, buf, _, b = path
        h = early[way]
        return copy(
            (name, "f2", way, d), buf.at[landing[way] * 4 + d, half[h]],
            buf.at[8 + d, half[h]], nb[b, way],
        )

    def send_p2(d):
        for k in range(2):
            for path in paths:
                for way in "RL":
                    start(p2(path, way, d, order[way][k]))

    def pass_p2(d):
        for path in paths:
            for way in "RL":
                p2(path, way, d, early[way]).wait_recv()
                start(f2(path, way, d))

    def rest_p2(d):
        for path in paths:
            for way in "RL":
                p2(path, way, d, 1 - early[way]).wait_recv()

    def wait_f2(d):
        for path in paths:
            for way in "RL":
                f2(path, way, d).wait_recv()

    m1 = {w: copy(("m", "p1", w), meta.at[0], meta.at[landing[w]], nb["z", w]) for w in "RL"}
    m1f = copy(("m", "f1"), meta.at[3], meta.at[2], nb["z", "R"])
    m2 = {
        w: copy(("m", "p2", w), meta.at[pl.ds(0, 4)], meta.at[pl.ds(4 * landing[w], 4)], nb["y", w])
        for w in "RL"
    }
    m2f = copy(("m", "f2"), meta.at[pl.ds(12, 4)], meta.at[pl.ds(8, 4)], nb["y", "R"])

    for w in "RL":
        start(m1[w])
    for k in range(2):
        for path in paths:
            for way in "RL":
                start(p1(path, way, order[way][k]))
    send_p2(0)

    zero = load(11, upv, up_out)

    @pl.when(sec == sections - 1)
    def _():
        upv[...] = jnp.zeros(upv.shape, BF)
        zero.start()
        zero.wait()

    upper[...] = jnp.where(
        lax.broadcasted_iota(jnp.int32, (T, T), 0) < lax.broadcasted_iota(jnp.int32, (T, T), 1), 1.0, 0.0
    ).astype(BF)

    def weight_grads(e):
        for c in saved(e):
            c.wait()
        row = lax.broadcasted_iota(jnp.int32, (SL, 1), 0)
        live = jnp.zeros((SL, 1), F32)
        for s in range(SL // cap):
            inside = (row >= s * cap) & (row < s * cap + cnt[e, s])
            live = jnp.where(inside, 1.0, live)
        for k in range(2):
            sgu[:, pl.ds(k * FF, FF)] = (sgu_raw[k].astype(F32) * live).astype(BF)
        if e > 0:
            for c in wout(e - 1):
                c.wait()
        width = min(256, D)

        def chunk(c, _):
            cols = pl.ds(pl.multiple_of(c * width, width), width)
            both = dot_tn(si[:, cols], sgu[...]).astype(BF)
            gov[cols, :] = both[:, :FF]
            uov[cols, :] = both[:, FF:]
            return 0

        lax.fori_loop(0, D // width, chunk, 0)
        for c in wout(e):
            c.start()
        if e + 1 < NE:
            for c in saved(e + 1):
                c.start()

    def prepare(i, _):
        m = meta[i].astype(F32)
        names, probs = m[:8], m[8:]
        row = lax.broadcasted_iota(jnp.int32, (8, T), 0)
        memb = jnp.zeros((8, T), F32)
        prob = jnp.zeros((8, T), F32)
        for e in range(NE):
            here = names == (ep * NE + e).astype(F32)
            me = jnp.max(jnp.where(here, 1.0, 0.0), axis=0, keepdims=True)
            pe = jnp.sum(jnp.where(here, probs, 0.0), axis=0, keepdims=True)
            memb = jnp.where(row == e, me, memb)
            prob = jnp.where(row == e + 4, pe, prob)
        rank = dot(memb.astype(BF), upper[...])
        slots[i] = jnp.where(row < 4, jnp.where(memb > 0.5, rank, -1.0), prob)
        return 0

    def batch(b):
        code = sum(i * 16**j for j, i in enumerate(BATCHES[b]))

        def dispatch(j, p):
            i = lax.rem(lax.div(jnp.int32(code), p), 16)
            it = lax.rem(i, 4) * 4 + lax.div(i, 4)
            spot = lax.broadcasted_iota(jnp.int32, (pad, T), 0).astype(F32)
            rows = pl.ds(pl.multiple_of(j * pad, pad), pad)
            for e in range(NE):
                hit = spot == slots[i, e : e + 1, :]
                oh[i, e * pad : (e + 1) * pad, :] = jnp.where(hit, 1.0, 0.0).astype(BF)
                weight = jnp.sum(
                    jnp.where(hit, slots[i, e + 4 : e + 5, :], 0.0), axis=1, keepdims=True
                )
                pv[e, rows, :] = jnp.broadcast_to(weight, (pad, 128))
            pick = oh[i]
            gx = dot(pick, gbuf[i]).astype(BF)
            for e in range(NE):
                gd[e, rows, :] = gx[e * pad : (e + 1) * pad]
            xx = dot(pick, xbuf[it]).astype(BF)
            for e in range(NE):
                xd[e, rows, :] = xx[e * pad : (e + 1) * pad]
            return p * 16

        lax.fori_loop(0, 4, dispatch, jnp.int32(1))

        def expert(e, _):
            gate = dot(xd[e], wg[e])
            up = dot(xd[e], wu[e])
            hg = dot_nt(gd[e], wd[e])
            sigma = jax.nn.sigmoid(gate)
            active = gate * sigma
            hidden = (active * up).astype(BF).astype(F32)
            slot_prob = jnp.sum(hidden * hg, axis=1, keepdims=True)
            sp[e] = jnp.broadcast_to(slot_prob, sp.shape[1:])
            scaled = hg * pv[e][:, :1]
            gg = (scaled * up * sigma * (1.0 + gate * (1.0 - sigma))).astype(BF)
            ug = (scaled * active).astype(BF)
            xd[e] = (dot_nt(gg, wg[e]) + dot_nt(ug, wu[e])).astype(BF)
            return 0

        lax.fori_loop(0, NE, expert, 0)

        def combine(j, p):
            i = lax.rem(lax.div(jnp.int32(code), p), 16)
            it = lax.rem(i, 4) * 4 + lax.div(i, 4)
            rows = pl.ds(pl.multiple_of(j * pad, pad), pad)
            part = jnp.concatenate([xd[e, rows, :] for e in range(NE)], axis=0)
            summed = dot_tn(oh[i], part).astype(BF)
            pa[i] = summed[:, :HD]
            pb[it] = summed[:, HD:]
            spot = lax.broadcasted_iota(jnp.int32, (pad, T), 0).astype(F32)
            names = meta[i].astype(F32)[:8]
            out = jnp.zeros((8, T), F32)
            for e in range(NE):
                hit = spot == slots[i, e : e + 1, :]
                val = jnp.sum(jnp.where(hit, sp[e, rows, :][:, :1], 0.0), axis=0, keepdims=True)
                out = jnp.where(names == (ep * NE + e).astype(F32), val, out)
            ppg[i] = out
            return p * 16

        lax.fori_loop(0, 4, combine, jnp.int32(1))

    halves = (("a", pa, "y", "z", 0), ("b", pb, "z", "y", 1))

    def source(hv, da, db):
        return da * 4 + db if hv[0] == "a" else db * 4 + da

    def far(hv, way, db):
        name, part, a, _, n = hv
        h = early[way]
        return copy(
            (name, "far", way, db), part.at[8 + db, half[h]],
            s1.at[n, 0 if way == "R" else 1, db], nb[a, way],
        )

    def near(hv, way, db, h):
        name, part, a, _, n = hv
        k = 0 if way == "R" else 1
        return copy(
            (name, "near", way, db, h), part.at[(1 if way == "R" else 3) * 4 + db, half[h]],
            fin.at[n, k, db, half[h]], nb[a, way],
        )

    def far2(hv, way):
        name, _, _, b, n = hv
        h = early[way]
        return copy(
            (name, "far2", way), q.at[n, 2, half[h]], t1.at[n, 0 if way == "R" else 1], nb[b, way]
        )

    def near2(hv, way, h):
        name, _, _, b, n = hv
        k = 0 if way == "R" else 1
        return copy(
            (name, "near2", way, h), q.at[n, 1 if way == "R" else 3, half[h]],
            gin.at[n, k, half[h]], nb[b, way],
        )

    issued = set()

    def issue_ready(b, dbs):
        for db in dbs:
            for hv in halves:
                if ("f", hv[0], db) not in issued and DONE_IN[source(hv, 2, db)] <= b:
                    issued.add(("f", hv[0], db))
                    for way in "RL":
                        start(far(hv, way, db))
        for db in dbs:
            for hv in halves:
                for way in "RL":
                    da = 1 if way == "R" else 3
                    if ("n", hv[0], way, db) not in issued and DONE_IN[source(hv, da, db)] <= b:
                        issued.add(("n", hv[0], way, db))
                        start(near(hv, way, db, 1 - early[way]))

    def merge(hv, db):
        _, part, _, _, n = hv
        for way in "RL":
            h = early[way]
            k, da = (0, 1) if way == "R" else (1, 3)
            far(hv, way, db).wait_recv()
            part[da * 4 + db, half[h], :] = (
                part[da * 4 + db, half[h], :].astype(F32) + s1[n, k, db].astype(F32)
            ).astype(BF)
            start(near(hv, way, db, h))

    def total(hv, db):
        _, part, _, _, n = hv
        for way in "RL":
            for h in range(2):
                near(hv, way, db, h).wait_recv()
        return part[db].astype(F32) + fin[n, 0, db].astype(F32) + fin[n, 1, db].astype(F32)

    weight_grads(0)
    for w in "RL":
        m1[w].wait_recv()
    start(m1f)
    for path in paths:
        for way in "RL":
            p1(path, way, early[way]).wait_recv()
            start(f1(path, way))
    for path in paths:
        for way in "RL":
            p1(path, way, 1 - early[way]).wait_recv()
    m1f.wait_recv()
    for w in "RL":
        start(m2[w])
    send_p2(1)
    send_p2(3)
    weight_grads(1)
    m2["R"].wait_recv()
    start(m2f)
    weight_grads(2)
    pass_p2(0)
    for path in paths:
        for way in "RL":
            f1(path, way).wait_recv()
    send_p2(2)
    weight_grads(3)
    m2["L"].wait_recv()
    m2f.wait_recv()
    lax.fori_loop(0, 16, prepare, 0)
    for c in weights:
        c.wait()
    rest_p2(0)
    batch(0)
    pass_p2(1)
    pass_p2(3)
    rest_p2(1)
    rest_p2(3)
    batch(1)
    pass_p2(2)
    issue_ready(1, (1, 2, 3, 0))
    rest_p2(2)
    wait_f2(0)
    wait_f2(1)
    batch(2)
    issue_ready(2, (1, 2, 3, 0))
    wait_f2(3)
    wait_f2(2)
    batch(3)

    c1 = copy(("c", 1), ppg.at[pl.ds(8, 4)], ppgr.at[0], nb["y", "R"])
    cl = copy(("c", 2), ppg.at[pl.ds(4, 4)], ppgr.at[1], nb["y", "R"])
    cr = copy(("c", 3), ppg.at[pl.ds(12, 4)], ppgr.at[2], nb["y", "L"])
    c2 = copy(("c", 4), ppg.at[2], ppgt.at[0], nb["z", "R"])
    cl2 = copy(("c", 5), ppg.at[1], ppgt.at[1], nb["z", "R"])
    cr2 = copy(("c", 6), ppg.at[3], ppgt.at[2], nb["z", "L"])
    start(c1)
    start(cr)
    issue_ready(3, (2, 1, 3, 0))
    c1.wait_recv()
    ppg[pl.ds(4, 4)] = ppg[pl.ds(4, 4)] + ppgr[0]
    start(cl)
    for db in (1, 2, 3, 0):
        for hv in halves:
            merge(hv, db)
    cl.wait_recv()
    cr.wait_recv()
    ppg[pl.ds(0, 4)] = ppg[pl.ds(0, 4)] + ppgr[1] + ppgr[2]
    start(c2)
    start(cr2)
    for db in (2, 1, 3):
        for hv in halves:
            q[hv[4], db] = total(hv, db).astype(BF)
            for way in "RL":
                if db == 2:
                    start(far2(hv, way))
                elif db == (1 if way == "R" else 3):
                    start(near2(hv, way, 1 - early[way]))
    c2.wait_recv()
    ppg[1] = ppg[1] + ppgt[0]
    start(cl2)
    for hv in halves:
        n = hv[4]
        for way in "RL":
            h = early[way]
            k, db = (0, 1) if way == "R" else (1, 3)
            far2(hv, way).wait_recv()
            q[n, db, half[h], :] = (q[n, db, half[h], :].astype(F32) + t1[n, k].astype(F32)).astype(BF)
            start(near2(hv, way, h))
    cl2.wait_recv()
    cr2.wait_recv()
    pg_out[...] = ppg[0] + ppgt[1] + ppgt[2]
    ups = [
        copy(("up", n), upv.at[:, pl.ds(n * HD, HD)], up_out.at[:, pl.ds(n * HD, HD)], before)
        for n in range(2)
    ]
    for hv in halves:
        n = hv[4]
        res = total(hv, 0)
        for way in "RL":
            for h in range(2):
                near2(hv, way, h).wait_recv()
        res = res + gin[n, 0].astype(F32) + gin[n, 1].astype(F32)
        upv[:, pl.ds(n * HD, HD)] = res.astype(BF)

        @pl.when(sec > 0)
        def _():
            ups[n].start()

    for c in wout(NE - 1):
        c.wait()
    for c in sent:
        c.wait_send()
    for n in range(2):
        @pl.when(sec > 0)
        def _():
            ups[n].wait_send()

        @pl.when(sec < sections - 1)
        def _():
            ups[n].wait_recv()


def per_device(sections, og, li, ids, probs, wg, wu, wd, si, sg, su, counts):
    T, D = og.shape[1], og.shape[2]
    NE, FF = wg.shape[1], wg.shape[3]
    SL = si.shape[2]
    cap = SL // 16
    pad = -(-cap // 16) * 16
    M = 4 * pad
    HD, H = D // 2, T // 2
    meta = jnp.concatenate([ids[0].T.astype(BF), probs[0].T], axis=0)
    hbm = pl.BlockSpec(memory_space=pl.ANY)
    V = pltpu.VMEM
    up, pg, go, uo = pl.pallas_call(
        functools.partial(kernel, sections, cap, pad),
        out_shape=(
            jax.ShapeDtypeStruct((T, D), BF),
            jax.ShapeDtypeStruct((8, T), F32),
            jax.ShapeDtypeStruct((NE, D, FF), BF),
            jax.ShapeDtypeStruct((NE, D, FF), BF),
        ),
        in_specs=[hbm] * 9 + [pl.BlockSpec(memory_space=pltpu.SMEM)],
        out_specs=(hbm, pl.BlockSpec(memory_space=V), hbm, hbm),
        scratch_shapes=[
            V((16, T, D), BF), V((16, T, D), BF), V((16, 16, T), BF),
            V((NE, D, FF), BF), V((NE, D, FF), BF), V((NE, FF, D), BF),
            V((SL, D), BF), V((2, SL, FF), BF), V((SL, 2 * FF), BF), V((D, FF), BF), V((D, FF), BF),
            V((16, 8, T), F32), V((T, T), BF), V((16, M, T), BF),
            V((NE, M, D), BF), V((NE, M, D), BF), V((NE, M, 128), F32), V((NE, M, 128), F32),
            V((16, T, HD), BF), V((16, T, HD), BF),
            V((2, 2, 4, H, HD), BF), V((2, 2, 4, T, HD), BF), V((2, 4, T, HD), BF),
            V((2, 2, H, HD), BF), V((2, 2, T, HD), BF), V((T, D), BF),
            V((16, 8, T), F32), V((3, 4, 8, T), F32), V((3, 8, T), F32),
            pltpu.SemaphoreType.DMA((N_SEMS,)), pltpu.SemaphoreType.DMA((N_SEMS,)),
            pltpu.SemaphoreType.DMA((12,)),
        ],
        compiler_params=pltpu.CompilerParams(
            collective_id=0, has_side_effects=True, vmem_limit_bytes=67_000_000
        ),
    )(og[0], li[0], meta, wg[0], wu[0], wd[0], si[0], sg[0], su[0], counts[0])
    return up[None], pg.T.astype(BF)[None], go[None], uo[None]


def solution(mesh):
    return jax.shard_map(
        functools.partial(per_device, mesh.shape["section"]),
        mesh=mesh,
        in_specs=(
            P("section", "ep", None),
            P("section", "ep", None),
            P("section", "ep", None),
            P("section", "ep", None),
            P("section", "ep", None, None),
            P("section", "ep", None, None),
            P("section", "ep", None, None),
            P("section", "ep", None, None),
            P("section", "ep", None, None),
            P("section", "ep", None, None),
            P("section", "ep", None),
        ),
        out_specs=(
            P("section", "ep", None),
            P("section", "ep", None),
            P("section", "ep", None, None),
            P("section", "ep", None, None),
        ),
        check_vma=False,
    )
```

```python
import functools

import jax
import jax.numpy as jnp
from jax import lax
from jax.experimental import pallas as pl
from jax.experimental.pallas import tpu as pltpu
from jax.sharding import PartitionSpec as P

MESH = pl.DeviceIdType.MESH
BF = jnp.bfloat16
F32 = jnp.float32

BATCHES = ((0, 4, 12, 1), (3, 5, 7, 13), (15, 8, 2, 9), (6, 11, 14, 10))
DONE_IN = {i: b for b, batch in enumerate(BATCHES) for i in batch}
N_SEMS = 160
WAYS = ("R", "L")


def dot(a, b):
    return jnp.dot(a, b, preferred_element_type=F32)


def dot_nt(a, b):
    return lax.dot_general(a, b, (((1,), (1,)), ((), ())), preferred_element_type=F32)


def dot_tn(a, b):
    return lax.dot_general(a, b, (((0,), (0,)), ((), ())), preferred_element_type=F32)


def kernel(
    sections, cap, pad,
    g_in, x_in, m_in, wg_in, wu_in, wd_in, si_in, sg_in, su_in, cnt,
    up_out, pg_out, go_out, uo_out,
    raw, cmp, sendc, relayc, meta, wg, wu, wd,
    si, sgu_raw, sgu, gov, uov,
    memb, slots, upper, oh, xg, pv, sp, srows,
    fr, nc, pm, nm, q, t1, gin, facc, upv, ppg, ppgr,
    ssem, rsem, lsem,
):
    T, HD = raw.shape[2], raw.shape[3]
    D = 2 * HD
    NE, FF = wg.shape[0], wg.shape[2]
    SL = si.shape[0]
    H = T // 2
    QD = HD // 2
    M = NE * cap
    half = (pl.ds(0, H), pl.ds(H, H))
    sec = lax.axis_index("section")
    ep = lax.axis_index("ep")
    y, z = lax.div(ep, 4), lax.rem(ep, 4)

    def at(yy, zz):
        return {"ep": lax.rem(yy, 4) * 4 + lax.rem(zz, 4)}

    nb = {
        ("y", 0): at(y + 1, z), ("y", 1): at(y + 3, z),
        ("z", 0): at(y, z + 1), ("z", 1): at(y, z + 3),
    }
    peers = {i: at(y + i // 4, z + i % 4) for i in range(1, 16)}
    mirror = {i: (4 - i // 4) % 4 * 4 + (4 - i % 4) % 4 for i in range(1, 16)}
    before = {"section": lax.rem(sec + sections - 1, sections)}
    after = {"section": lax.rem(sec + 1, sections)}

    ids = {}
    sent = []

    def copy(key, src, dst, dev):
        k = ids.setdefault(key, len(ids))
        return pltpu.make_async_remote_copy(
            src_ref=src, dst_ref=dst, send_sem=ssem.at[k], recv_sem=rsem.at[k],
            device_id=dev, device_id_type=MESH,
        )

    def start(c):
        c.start()
        sent.append(c)

    def load(k, src, dst):
        return pltpu.make_async_copy(src, dst, lsem.at[k])

    own = [load(0, m_in, meta.at[0])] + [
        load(1 + 2 * p + ch, ref.at[:, pl.ds(ch * HD, HD)], raw.at[p, ch])
        for p, ref in enumerate((g_in, x_in)) for ch in range(2)
    ]
    for c in own:
        c.start()
    weights = [load(5, wg_in, wg), load(6, wu_in, wu), load(7, wd_in, wd)]

    def saved(e):
        return [
            load(8, si_in.at[e], si),
            load(9, sg_in.at[e], sgu_raw.at[0]),
            load(10, su_in.at[e], sgu_raw.at[1]),
        ]

    def wout(e):
        return [load(11, gov, go_out.at[e]), load(12, uov, uo_out.at[e])]

    barrier = pltpu.get_barrier_semaphore()
    for dev in (*peers.values(), before, after):
        pl.semaphore_signal(barrier, inc=1, device_id=dev, device_id_type=MESH)
    for c in saved(0):
        c.start()
    for c in weights:
        c.start()
    pl.semaphore_wait(barrier, 17)
    for c in own:
        c.wait()

    axes = (("z", "y"), ("y", "z"))
    land = (3, 1)
    both = [(p, w) for p in range(2) for w in range(2)]

    def p1(p, w, ch):
        return copy((p, "p1", w, ch), raw.at[p, ch], raw.at[p, 2 * land[w] + ch], nb[axes[p][0], w])

    def f1(p, w):
        return copy(
            (p, "f1", w), raw.at[p, 2 * land[w] + w], raw.at[p, 4 + w], nb[axes[p][0], w]
        )

    def p2(p, w, d):
        return copy(
            (p, "p2", w, d), raw.at[p, 2 * d + 1 - w], raw.at[p, 8 + 4 * w + d], nb[axes[p][1], w]
        )

    def c2(p, w, d):
        return copy((p, "c2", w, d), sendc.at[p, w, d], cmp.at[p, 4 * w + d], nb[axes[p][1], w])

    def r2(p, w, d):
        return copy((p, "r2", w, d), relayc.at[p, w, d], cmp.at[p, 8 + 4 * w + d], nb[axes[p][1], w])

    def pair(axis, w, kind, d):
        return 16 + axis * 16 + w * 8 + kind * 4 + d

    def send_p2(d):
        for p, w in both:
            start(p2(p, w, d))

    def send_c2(d):
        def pick(n, _):
            p, w = lax.div(n, 2), lax.rem(n, 2)
            sendc[p, w, d] = dot(oh[pair(p, w, 0, d)], raw[p, 2 * d + w]).astype(BF)
            return 0

        lax.fori_loop(0, 4, pick, 0)
        for p, w in both:
            start(c2(p, w, d))

    def relay(d):
        for p, w in both:
            p2(p, w, d).wait_recv()

        def pick(n, _):
            p, w = lax.div(n, 2), lax.rem(n, 2)
            relayc[p, w, d] = dot(oh[pair(p, w, 1, d)], raw[p, 8 + 4 * w + d]).astype(BF)
            return 0

        lax.fori_loop(0, 4, pick, 0)
        for p, w in both:
            start(r2(p, w, d))

    def wait_c2(d):
        for p, w in both:
            c2(p, w, d).wait_recv()

    def wait_r2(d):
        for p, w in both:
            r2(p, w, d).wait_recv()

    ms = [copy(("m", i), meta.at[0], meta.at[mirror[i]], peers[i]) for i in range(1, 16)]
    for c in ms:
        start(c)
    for k in range(2):
        for p, w in both:
            start(p1(p, w, w if k == 0 else 1 - w))
    send_p2(0)

    zero = load(13, upv, up_out)

    @pl.when(sec == sections - 1)
    def _():
        upv[...] = jnp.zeros(upv.shape, BF)
        zero.start()
        zero.wait()

    upper[...] = jnp.where(
        lax.broadcasted_iota(jnp.int32, (T, T), 0) < lax.broadcasted_iota(jnp.int32, (T, T), 1), 1.0, 0.0
    ).astype(BF)
    pv[...] = jnp.zeros(pv.shape, F32)

    def weight_grads(e):
        for c in saved(e):
            c.wait()
        row = lax.broadcasted_iota(jnp.int32, (SL, 1), 0)
        live = jnp.zeros((SL, 1), F32)
        for s in range(SL // cap):
            inside = (row >= s * cap) & (row < s * cap + cnt[e, s])
            live = jnp.where(inside, 1.0, live)
        for k in range(2):
            sgu[:, pl.ds(k * FF, FF)] = (sgu_raw[k].astype(F32) * live).astype(BF)
        if e > 0:
            for c in wout(e - 1):
                c.wait()
        width = min(256, D)

        def chunk(c, _):
            cols = pl.ds(pl.multiple_of(c * width, width), width)
            res = dot_tn(si[:, cols], sgu[...]).astype(BF)
            gov[cols, :] = res[:, :FF]
            uov[cols, :] = res[:, FF:]
            return 0

        lax.fori_loop(0, D // width, chunk, 0)
        for c in wout(e):
            c.start()
        if e + 1 < NE:
            for c in saved(e + 1):
                c.start()

    def member(n, i, owner):
        m = meta[i].astype(F32)
        names, probs = m[:8], m[8:]
        row = lax.broadcasted_iota(jnp.int32, (8, T), 0)
        is_in = jnp.zeros((8, T), F32)
        prob = jnp.zeros((8, T), F32)
        for e in range(NE):
            here = names == (owner * NE + e).astype(F32)
            me = jnp.max(jnp.where(here, 1.0, 0.0), axis=0, keepdims=True)
            pe = jnp.sum(jnp.where(here, probs, 0.0), axis=0, keepdims=True)
            is_in = jnp.where(row == e, me, is_in)
            prob = jnp.where(row == e + 4, pe, prob)
        memb[n] = is_in
        slots[n] = prob

    def member_self(n, _):
        member(n, n, ep)
        return 0

    def member_near(m, _):
        axis, w, kind, d = lax.div(m, 16), lax.rem(lax.div(m, 8), 2), lax.rem(lax.div(m, 4), 2), lax.rem(m, 4)
        d2 = kind * (3 - 2 * w)
        i = (1 - axis) * (d2 * 4 + d) + axis * (d * 4 + d2)
        step = 1 + 2 * w
        owner = lax.rem(y + (1 - axis) * step, 4) * 4 + lax.rem(z + axis * step, 4)
        member(16 + m, i, owner)
        return 0

    def one_hot(n, _):
        spot = lax.broadcasted_iota(jnp.int32, (cap, T), 0).astype(F32)
        rows = [jnp.where(spot == slots[n, e : e + 1, :], 1.0, 0.0) for e in range(NE)]
        oh[n] = jnp.concatenate(rows, axis=0).astype(BF)
        return 0

    def prepare():
        lax.fori_loop(0, 16, member_self, 0)
        lax.fori_loop(0, 32, member_near, 0)
        inside = memb[...].reshape(48 * 8, T)
        rank = dot(inside.astype(BF), upper[...])
        row = lax.rem(lax.broadcasted_iota(jnp.int32, (48 * 8, T), 0), 8)
        prob = slots[...].reshape(48 * 8, T)
        slots[...] = jnp.where(row < 4, jnp.where(inside > 0.5, rank, -1.0), prob).reshape(48, 8, T)
        lax.fori_loop(0, 48, one_hot, 0)

    def place(p, j, cols, v):
        for k in range(NE // 2):
            xg[p, 2 * k, pl.ds(j * pad, pad), cols] = v[2 * cap * k : 2 * cap * k + pad]
            xg[p, 2 * k + 1, pl.ds(j * pad, pad), cols] = v[2 * cap * (k + 1) - pad : 2 * cap * (k + 1)]

    def dispatch(p, i, j):
        d2, d = (i // 4, i % 4) if p == 0 else (i % 4, i // 4)
        low, high = pl.ds(0, HD), pl.ds(HD, HD)
        if d2 == 0:
            def pick(ch, _):
                cols = pl.ds(pl.multiple_of(ch * HD, HD), HD)
                place(p, j, cols, dot(oh[i], raw[p, 2 * d + ch]).astype(BF))
                return 0

            lax.fori_loop(0, 2, pick, 0)
        elif d2 == 3:
            place(p, j, high, dot(oh[i], raw[p, 8 + d]).astype(BF))
            place(p, j, low, cmp[p, d])
        elif d2 == 1:
            place(p, j, low, dot(oh[i], raw[p, 12 + d]).astype(BF))
            place(p, j, high, cmp[p, 4 + d])
        else:
            place(p, j, high, cmp[p, 8 + d])
            place(p, j, low, cmp[p, 12 + d])

    def batch(b):
        code = sum(i * 16**j for j, i in enumerate(BATCHES[b]))
        for j, i in enumerate(BATCHES[b]):
            for p in range(2):
                dispatch(p, i, j)

        def weigh(j, t):
            i = lax.rem(lax.div(jnp.int32(code), t), 16)
            spot = lax.broadcasted_iota(jnp.int32, (cap, T), 0).astype(F32)
            for e in range(NE):
                hit = spot == slots[i, e : e + 1, :]
                weight = jnp.sum(
                    jnp.where(hit, slots[i, e + 4 : e + 5, :], 0.0), axis=1, keepdims=True
                )
                rows = pl.ds(pl.multiple_of(j * pad + e % 2 * (pad - cap), 8), cap)
                pv[e, rows, :] = jnp.broadcast_to(weight, (cap, 128))
            return t * 16

        lax.fori_loop(0, 4, weigh, jnp.int32(1))

        def expert(e, _):
            gate = dot(xg[1, e], wg[e])
            up = dot(xg[1, e], wu[e])
            hg = dot_nt(xg[0, e], wd[e])
            sigma = jax.nn.sigmoid(gate)
            active = gate * sigma
            hidden = (active * up).astype(BF).astype(F32)
            slot_prob = jnp.sum(hidden * hg, axis=1, keepdims=True)
            sp[e] = jnp.broadcast_to(slot_prob, sp.shape[1:])
            scaled = hg * pv[e][:, :1]
            gg = (scaled * up * sigma * (1.0 + gate * (1.0 - sigma))).astype(BF)
            ug = (scaled * active).astype(BF)
            xg[1, e] = (dot_nt(gg, wg[e]) + dot_nt(ug, wu[e])).astype(BF)
            return 0

        lax.fori_loop(0, NE, expert, 0)

        def finish(j, t):
            i = lax.rem(lax.div(jnp.int32(code), t), 16)
            rows = pl.ds(pl.multiple_of(j * pad, pad), pad)
            cut = cap // 16 * 16
            for k in range(NE // 2):
                even, odd = xg[1, 2 * k, rows, :], xg[1, 2 * k + 1, rows, :]
                middle = jnp.concatenate(
                    [even[cut:].astype(F32)[:8], odd[:16].astype(F32)[8:]], axis=0
                ).astype(BF)
                o = 2 * cap * k
                srows[i, o : o + cut, :] = even[:cut]
                srows[i, o + cut : o + cut + 16, :] = middle
                srows[i, o + cut + 16 : o + 2 * cap, :] = odd[16:]
            spot = lax.broadcasted_iota(jnp.int32, (cap, T), 0).astype(F32)
            names = meta[i].astype(F32)[:8]
            out = jnp.zeros((8, T), F32)
            for e in range(NE):
                hit = spot == slots[i, e : e + 1, :]
                part = pl.ds(pl.multiple_of(j * pad + e % 2 * (pad - cap), 8), cap)
                val = jnp.sum(jnp.where(hit, sp[e, part, :][:, :1], 0.0), axis=0, keepdims=True)
                out = jnp.where(names == (ep * NE + e).astype(F32), val, out)
            ppg[i] = out
            return t * 16

        lax.fori_loop(0, 4, finish, jnp.int32(1))

    lead = (("y", "z"), ("z", "y"))

    def source(h, da, db):
        return da * 4 + db if h == 0 else db * 4 + da

    def far(h, w, db):
        return copy(
            ("far", h, w, db), srows.at[source(h, 2, db), :, pl.ds(h * HD + w * QD, QD)],
            fr.at[h, w, db], nb[lead[h][0], w],
        )

    def nearc(h, w, db):
        return copy(
            ("nc", h, w, db), srows.at[source(h, 1 + 2 * w, db), :, pl.ds(h * HD + (1 - w) * QD, QD)],
            nc.at[h, w, db], nb[lead[h][0], w],
        )

    def nearm(h, w, db):
        return copy(("nm", h, w, db), pm.at[h, w, db], nm.at[h, w, db], nb[lead[h][0], w])

    def far2(h, w):
        return copy(("far2", h, w), q.at[h, 2, half[w]], t1.at[h, w], nb[lead[h][1], w])

    def near2(h, w, k):
        return copy(
            ("near2", h, w, k), q.at[h, 1 + 2 * w, half[k]], gin.at[h, w, half[k]], nb[lead[h][1], w]
        )

    issued = set()

    def issue_ready(b, dbs):
        for kind in ("far", "near"):
            for db in dbs:
                for h, w in both:
                    da = 2 if kind == "far" else 1 + 2 * w
                    if (kind, h, w, db) not in issued and DONE_IN[source(h, da, db)] <= b:
                        issued.add((kind, h, w, db))
                        start((far if kind == "far" else nearc)(h, w, db))

    def merge(db):
        for h, w in both:
            far(h, w, db).wait_recv()

        def add(n, _):
            h, w = lax.div(n, 2), lax.rem(n, 2)
            da = 1 + 2 * w
            i = (1 - h) * (da * 4 + db) + h * (db * 4 + da)
            cols = pl.ds(pl.multiple_of(h * HD + w * QD, QD), QD)
            lhs = jnp.concatenate([oh[i], oh[pair(h, 1 - w, 1, db)]], axis=0)
            rhs = jnp.concatenate([srows[i, :, cols], fr[h, w, db]], axis=0)
            pm[h, w, db] = dot_tn(lhs, rhs).astype(BF)
            return 0

        lax.fori_loop(0, 4, add, 0)
        for h, w in both:
            start(nearm(h, w, db))

    def total(db):
        for h, w in both:
            nearc(h, w, db).wait_recv()
            nearm(h, w, db).wait_recv()

        def add(n, _):
            h, k = lax.div(n, 2), lax.rem(n, 2)
            i = (1 - h) * db + h * (db * 4)
            cols = pl.ds(pl.multiple_of(h * HD + k * QD, QD), QD)
            lhs = jnp.concatenate([oh[i], oh[pair(h, k, 0, db)]], axis=0)
            rhs = jnp.concatenate([srows[i, :, cols], nc[h, 1 - k, db]], axis=0)
            res = dot_tn(lhs, rhs) + nm[h, k, db].astype(F32)
            part = pl.ds(pl.multiple_of(k * QD, QD), QD)
            if db == 0:
                facc[h, :, part] = res
            else:
                q[h, db, :, part] = res.astype(BF)
            return 0

        lax.fori_loop(0, 4, add, 0)

    weight_grads(0)
    for c in ms:
        c.wait_recv()
    prepare()
    send_c2(0)
    for p, w in both:
        p1(p, w, w).wait_recv()
        start(f1(p, w))
    for p, w in both:
        p1(p, w, 1 - w).wait_recv()
    send_p2(1)
    send_p2(3)
    send_c2(1)
    send_c2(3)
    weight_grads(1)
    relay(0)
    for p, w in both:
        f1(p, w).wait_recv()
    send_p2(2)
    send_c2(2)
    weight_grads(2)
    for c in weights:
        c.wait()
    wait_c2(0)
    batch(0)
    relay(1)
    relay(3)
    weight_grads(3)
    wait_c2(1)
    wait_c2(3)
    batch(1)
    relay(2)
    issue_ready(1, (1, 2, 3, 0))
    wait_c2(2)
    wait_r2(0)
    wait_r2(1)
    batch(2)
    issue_ready(2, (1, 2, 3, 0))
    wait_r2(3)
    wait_r2(2)
    batch(3)
    issue_ready(3, (2, 1, 3, 0))
    pgs = [copy(("c", i), ppg.at[i], ppgr.at[mirror[i]], peers[i]) for i in range(1, 16)]
    for c in pgs:
        start(c)
    for db in (1, 2, 3, 0):
        merge(db)
    total(2)
    for h, w in both:
        start(far2(h, w))
    total(1)
    total(3)
    for h, w in both:
        start(near2(h, w, 1 - w))
    total(0)
    for h, w in both:
        db = 1 + 2 * w
        far2(h, w).wait_recv()
        q[h, db, half[w], :] = (q[h, db, half[w], :].astype(F32) + t1[h, w].astype(F32)).astype(BF)
        start(near2(h, w, w))
    for c in pgs:
        c.wait_recv()
    routed = ppg[0]
    for i in range(1, 16):
        routed = routed + ppgr[i]
    pg_out[...] = routed
    ups = [
        copy(("up", h), upv.at[:, pl.ds(h * HD, HD)], up_out.at[:, pl.ds(h * HD, HD)], before)
        for h in range(2)
    ]
    for h in range(2):
        for w in range(2):
            for k in range(2):
                near2(h, w, k).wait_recv()
        upv[:, pl.ds(h * HD, HD)] = (
            facc[h] + gin[h, 0].astype(F32) + gin[h, 1].astype(F32)
        ).astype(BF)

        @pl.when(sec > 0)
        def _():
            ups[h].start()

    for c in wout(NE - 1):
        c.wait()
    for c in sent:
        c.wait_send()
    for h in range(2):
        @pl.when(sec > 0)
        def _():
            ups[h].wait_send()

        @pl.when(sec < sections - 1)
        def _():
            ups[h].wait_recv()


def per_device(sections, og, li, ids, probs, wg, wu, wd, si, sg, su, counts):
    T, D = og.shape[1], og.shape[2]
    NE, FF = wg.shape[1], wg.shape[3]
    SL = si.shape[2]
    cap = SL // 16
    pad = -(-cap // 16) * 16
    M, R = NE * cap, 4 * pad
    HD, QD, H = D // 2, D // 4, T // 2
    meta = jnp.concatenate([ids[0].T.astype(BF), probs[0].T], axis=0)
    hbm = pl.BlockSpec(memory_space=pl.ANY)
    V = pltpu.VMEM
    up, pg, go, uo = pl.pallas_call(
        functools.partial(kernel, sections, cap, pad),
        out_shape=(
            jax.ShapeDtypeStruct((T, D), BF),
            jax.ShapeDtypeStruct((8, T), F32),
            jax.ShapeDtypeStruct((NE, D, FF), BF),
            jax.ShapeDtypeStruct((NE, D, FF), BF),
        ),
        in_specs=[hbm] * 9 + [pl.BlockSpec(memory_space=pltpu.SMEM)],
        out_specs=(hbm, pl.BlockSpec(memory_space=V), hbm, hbm),
        scratch_shapes=[
            V((2, 16, T, HD), BF), V((2, 16, M, HD), BF), V((2, 2, 4, M, HD), BF), V((2, 2, 4, M, HD), BF),
            V((16, 16, T), BF), V((NE, D, FF), BF), V((NE, D, FF), BF), V((NE, FF, D), BF),
            V((SL, D), BF), V((2, SL, FF), BF), V((SL, 2 * FF), BF), V((D, FF), BF), V((D, FF), BF),
            V((48, 8, T), F32), V((48, 8, T), F32), V((T, T), BF), V((48, M, T), BF),
            V((2, NE, R, D), BF), V((NE, R, 128), F32), V((NE, R, 128), F32), V((16, M, D), BF),
            V((2, 2, 4, M, QD), BF), V((2, 2, 4, M, QD), BF),
            V((2, 2, 4, T, QD), BF), V((2, 2, 4, T, QD), BF),
            V((2, 4, T, HD), BF), V((2, 2, H, HD), BF), V((2, 2, T, HD), BF), V((2, T, HD), F32),
            V((T, D), BF), V((16, 8, T), F32), V((16, 8, T), F32),
            pltpu.SemaphoreType.DMA((N_SEMS,)), pltpu.SemaphoreType.DMA((N_SEMS,)),
            pltpu.SemaphoreType.DMA((14,)),
        ],
        compiler_params=pltpu.CompilerParams(
            collective_id=0, has_side_effects=True, vmem_limit_bytes=67_000_000
        ),
    )(og[0], li[0], meta, wg[0], wu[0], wd[0], si[0], sg[0], su[0], counts[0])
    return up[None], pg.T.astype(BF)[None], go[None], uo[None]


def solution(mesh):
    return jax.shard_map(
        functools.partial(per_device, mesh.shape["section"]),
        mesh=mesh,
        in_specs=(
            P("section", "ep", None),
            P("section", "ep", None),
            P("section", "ep", None),
            P("section", "ep", None),
            P("section", "ep", None, None),
            P("section", "ep", None, None),
            P("section", "ep", None, None),
            P("section", "ep", None, None),
            P("section", "ep", None, None),
            P("section", "ep", None, None),
            P("section", "ep", None),
        ),
        out_specs=(
            P("section", "ep", None),
            P("section", "ep", None),
            P("section", "ep", None, None),
            P("section", "ep", None, None),
        ),
        check_vma=False,
    )
```

```python
import functools

import jax
import jax.numpy as jnp
from jax import lax
from jax.experimental import pallas as pl
from jax.experimental.pallas import tpu as pltpu
from jax.sharding import PartitionSpec as P

MESH = pl.DeviceIdType.MESH
BF = jnp.bfloat16
F32 = jnp.float32

BATCHES = ((4, 12, 1, 3), (8, 2, 5, 0), (7, 13, 15), (9, 6), (11, 14, 10))
DONE_IN = {i: b for b, batch in enumerate(BATCHES) for i in batch}
N_SEMS = 176
WAYS = ("R", "L")


def dot(a, b):
    return jnp.dot(a, b, preferred_element_type=F32)


def dot_nt(a, b):
    return lax.dot_general(a, b, (((1,), (1,)), ((), ())), preferred_element_type=F32)


def dot_tn(a, b):
    return lax.dot_general(a, b, (((0,), (0,)), ((), ())), preferred_element_type=F32)


def kernel(
    sections, cap, pad,
    g_in, x_in, ids_in, prob_in, wg_in, wu_in, wd_in, si_in, sg_in, su_in, cnt,
    up_out, pg_out, go_out, uo_out,
    raw, cmp, sendc, relayc, meta, wgu, wd,
    si, sgu_raw, sgu,
    memb, slots, upper, oh, xg, pv, sp, srows,
    fr, nc, pm, nm, q, t1, gin, facc, upv, ppg, ppgr,
    ssem, rsem, lsem,
):
    T, HD = raw.shape[2], raw.shape[3]
    D = 2 * HD
    NE, FF = wd.shape[0], wd.shape[1]
    SL = si.shape[0]
    H = T // 2
    QD = HD // 2
    M = NE * cap
    half = (pl.ds(0, H), pl.ds(H, H))
    sec = lax.axis_index("section")
    ep = lax.axis_index("ep")
    y, z = lax.div(ep, 4), lax.rem(ep, 4)

    def at(yy, zz):
        return {"ep": lax.rem(yy, 4) * 4 + lax.rem(zz, 4)}

    nb = {
        ("y", 0): at(y + 1, z), ("y", 1): at(y + 3, z),
        ("z", 0): at(y, z + 1), ("z", 1): at(y, z + 3),
    }
    peers = {i: at(y + i // 4, z + i % 4) for i in range(1, 16)}
    mirror = {i: (4 - i // 4) % 4 * 4 + (4 - i % 4) % 4 for i in range(1, 16)}
    before = {"section": lax.rem(sec + sections - 1, sections)}
    after = {"section": lax.rem(sec + 1, sections)}

    ids = {}
    sent = []

    def copy(key, src, dst, dev):
        k = ids.setdefault(key, len(ids))
        return pltpu.make_async_remote_copy(
            src_ref=src, dst_ref=dst, send_sem=ssem.at[k], recv_sem=rsem.at[k],
            device_id=dev, device_id_type=MESH,
        )

    def start(c):
        c.start()
        sent.append(c)

    def load(k, src, dst):
        return pltpu.make_async_copy(src, dst, lsem.at[k])

    own = [
        load(1 + 2 * p + ch, ref.at[:, pl.ds(ch * HD, HD)], raw.at[p, ch])
        for p, ref in enumerate((g_in, x_in)) for ch in range(2)
    ]
    for c in own:
        c.start()
    weights = [
        load(5, wg_in, wgu.at[:, :, pl.ds(0, FF)]),
        load(6, wu_in, wgu.at[:, :, pl.ds(FF, FF)]),
        load(7, wd_in, wd),
    ]

    def saved(e):
        return [
            load(8, si_in.at[e], si),
            load(9, sg_in.at[e], sgu_raw.at[0]),
            load(10, su_in.at[e], sgu_raw.at[1]),
        ]

    barrier = pltpu.get_barrier_semaphore()
    for dev in (*peers.values(), before, after):
        pl.semaphore_signal(barrier, inc=1, device_id=dev, device_id_type=MESH)
    for c in saved(0):
        c.start()
    for c in weights:
        c.start()
    meta[0] = jnp.concatenate([ids_in[...].astype(F32), prob_in[...].astype(F32)], axis=0).astype(BF)
    pl.semaphore_wait(barrier, 17)
    for c in own:
        c.wait()

    axes = (("z", "y"), ("y", "z"))
    land = (3, 1)
    both = [(p, w) for p in range(2) for w in range(2)]

    def p1(p, w, ch):
        return copy((p, "p1", w, ch), raw.at[p, ch], raw.at[p, 2 * land[w] + ch], nb[axes[p][0], w])

    def f1(p, w):
        return copy(
            (p, "f1", w), raw.at[p, 2 * land[w] + w], raw.at[p, 4 + w], nb[axes[p][0], w]
        )

    def p2(p, w, d):
        return copy(
            (p, "p2", w, d), raw.at[p, 2 * d + 1 - w], raw.at[p, 8 + 4 * w + d], nb[axes[p][1], w]
        )

    def c2(p, w, d):
        return copy((p, "c2", w, d), sendc.at[p, w, d], cmp.at[p, 4 * w + d], nb[axes[p][1], w])

    def r2(p, w, d):
        return copy((p, "r2", w, d), relayc.at[p, w, d], cmp.at[p, 8 + 4 * w + d], nb[axes[p][1], w])

    def pair(axis, w, kind, d):
        return 16 + axis * 16 + w * 8 + kind * 4 + d

    def send_p2(d):
        for p, w in both:
            start(p2(p, w, d))

    def send_c2(d):
        def pick(n, _):
            p, w = lax.div(n, 2), lax.rem(n, 2)
            sendc[p, w, d] = dot(oh[pair(p, w, 0, d)], raw[p, 2 * d + w]).astype(BF)
            return 0

        lax.fori_loop(0, 4, pick, 0)
        for p, w in both:
            start(c2(p, w, d))

    def relay(d):
        for p, w in both:
            p2(p, w, d).wait_recv()

        def pick(n, _):
            p, w = lax.div(n, 2), lax.rem(n, 2)
            relayc[p, w, d] = dot(oh[pair(p, w, 1, d)], raw[p, 8 + 4 * w + d]).astype(BF)
            return 0

        lax.fori_loop(0, 4, pick, 0)
        for p, w in both:
            start(r2(p, w, d))

    def wait_c2(d):
        for p, w in both:
            c2(p, w, d).wait_recv()

    def wait_r2(d):
        for p, w in both:
            r2(p, w, d).wait_recv()

    ms = [copy(("m", i), meta.at[0], meta.at[mirror[i]], peers[i]) for i in range(1, 16)]
    for c in ms:
        start(c)
    for k in range(2):
        for p, w in both:
            start(p1(p, w, w if k == 0 else 1 - w))
    send_p2(0)

    @pl.when(sec == sections - 1)
    def _():
        up_out[...] = jnp.zeros(up_out.shape, BF)

    upper[...] = jnp.where(
        lax.broadcasted_iota(jnp.int32, (T, T), 0) < lax.broadcasted_iota(jnp.int32, (T, T), 1), 1.0, 0.0
    ).astype(BF)
    pv[...] = jnp.zeros(pv.shape, F32)

    def weight_grads(e):
        for c in saved(e):
            c.wait()
        row = lax.broadcasted_iota(jnp.int32, (SL, 1), 0)
        live = jnp.zeros((SL, 1), F32)
        for s in range(SL // cap):
            inside = (row >= s * cap) & (row < s * cap + cnt[e, s])
            live = jnp.where(inside, 1.0, live)
        for k in range(2):
            sgu[:, pl.ds(k * FF, FF)] = (sgu_raw[k].astype(F32) * live).astype(BF)
        width = min(256, D)

        def chunk(c, _):
            cols = pl.ds(pl.multiple_of(c * width, width), width)
            res = dot_tn(si[:, cols], sgu[...]).astype(BF)
            go_out[e, cols, :] = res[:, :FF]
            uo_out[e, cols, :] = res[:, FF:]
            return 0

        lax.fori_loop(0, D // width, chunk, 0)
        if e + 1 < NE:
            for c in saved(e + 1):
                c.start()

    def member(n, i, owner):
        m = meta[i].astype(F32)
        names, probs = m[:8], m[8:]
        row = lax.broadcasted_iota(jnp.int32, (8, T), 0)
        is_in = jnp.zeros((8, T), F32)
        prob = jnp.zeros((8, T), F32)
        for e in range(NE):
            here = names == (owner * NE + e).astype(F32)
            me = jnp.max(jnp.where(here, 1.0, 0.0), axis=0, keepdims=True)
            pe = jnp.sum(jnp.where(here, probs, 0.0), axis=0, keepdims=True)
            is_in = jnp.where(row == e, me, is_in)
            prob = jnp.where(row == e + 4, pe, prob)
        memb[n] = is_in
        slots[n] = prob

    def member_self(n, _):
        member(n, n, ep)
        return 0

    def member_near(m, _):
        axis, w, kind, d = lax.div(m, 16), lax.rem(lax.div(m, 8), 2), lax.rem(lax.div(m, 4), 2), lax.rem(m, 4)
        d2 = kind * (3 - 2 * w)
        i = (1 - axis) * (d2 * 4 + d) + axis * (d * 4 + d2)
        step = 1 + 2 * w
        owner = lax.rem(y + (1 - axis) * step, 4) * 4 + lax.rem(z + axis * step, 4)
        member(16 + m, i, owner)
        return 0

    def one_hot(n, _):
        spot = lax.broadcasted_iota(jnp.int32, (cap, T), 0).astype(F32)
        rows = [jnp.where(spot == slots[n, e : e + 1, :], 1.0, 0.0) for e in range(NE)]
        oh[n] = jnp.concatenate(rows, axis=0).astype(BF)
        return 0

    def prepare():
        lax.fori_loop(0, 16, member_self, 0)
        lax.fori_loop(0, 32, member_near, 0)
        inside = memb[...].reshape(48 * 8, T)
        rank = dot(inside.astype(BF), upper[...])
        row = lax.rem(lax.broadcasted_iota(jnp.int32, (48 * 8, T), 0), 8)
        prob = slots[...].reshape(48 * 8, T)
        slots[...] = jnp.where(row < 4, jnp.where(inside > 0.5, rank, -1.0), prob).reshape(48, 8, T)
        lax.fori_loop(0, 48, one_hot, 0)

    def place(p, j, cols, v):
        for k in range(NE // 2):
            xg[p, 2 * k, pl.ds(j * pad, pad), cols] = v[2 * cap * k : 2 * cap * k + pad]
            xg[p, 2 * k + 1, pl.ds(j * pad, pad), cols] = v[2 * cap * (k + 1) - pad : 2 * cap * (k + 1)]

    def dispatch(p, i, j):
        d2, d = (i // 4, i % 4) if p == 0 else (i % 4, i // 4)
        low, high = pl.ds(0, HD), pl.ds(HD, HD)
        if d2 == 0:
            def pick(ch, _):
                cols = pl.ds(pl.multiple_of(ch * HD, HD), HD)
                place(p, j, cols, dot(oh[i], raw[p, 2 * d + ch]).astype(BF))
                return 0

            lax.fori_loop(0, 2, pick, 0)
        elif d2 == 3:
            place(p, j, high, dot(oh[i], raw[p, 8 + d]).astype(BF))
            place(p, j, low, cmp[p, d])
        elif d2 == 1:
            place(p, j, low, dot(oh[i], raw[p, 12 + d]).astype(BF))
            place(p, j, high, cmp[p, 4 + d])
        else:
            place(p, j, high, cmp[p, 8 + d])
            place(p, j, low, cmp[p, 12 + d])

    def batch(b):
        code = sum(i * 16**j for j, i in enumerate(BATCHES[b]))
        count = len(BATCHES[b])
        used = pl.ds(0, count * pad)
        for j, i in enumerate(BATCHES[b]):
            for p in range(2):
                dispatch(p, i, j)

        def weigh(j, t):
            i = lax.rem(lax.div(jnp.int32(code), t), 16)
            spot = lax.broadcasted_iota(jnp.int32, (cap, T), 0).astype(F32)
            for e in range(NE):
                hit = spot == slots[i, e : e + 1, :]
                weight = jnp.sum(
                    jnp.where(hit, slots[i, e + 4 : e + 5, :], 0.0), axis=1, keepdims=True
                )
                rows = pl.ds(pl.multiple_of(j * pad + e % 2 * (pad - cap), 8), cap)
                pv[e, rows, :] = jnp.broadcast_to(weight, (cap, 128))
            return t * 16

        lax.fori_loop(0, count, weigh, jnp.int32(1))

        def expert(e, _):
            gate_up = dot(xg[1, e, used, :], wgu[e])
            gate, up = gate_up[:, :FF], gate_up[:, FF:]
            hg = dot_nt(xg[0, e, used, :], wd[e])
            sigma = jax.nn.sigmoid(gate)
            active = gate * sigma
            hidden = (active * up).astype(BF).astype(F32)
            slot_prob = jnp.sum(hidden * hg, axis=1, keepdims=True)
            sp[e, used, :] = jnp.broadcast_to(slot_prob, (count * pad, 128))
            scaled = hg * pv[e, used, :][:, :1]
            gg = (scaled * up * sigma * (1.0 + gate * (1.0 - sigma))).astype(BF)
            ug = (scaled * active).astype(BF)
            xg[1, e, used, :] = dot_nt(jnp.concatenate([gg, ug], axis=1), wgu[e]).astype(BF)
            return 0

        lax.fori_loop(0, NE, expert, 0)

        def finish(j, t):
            i = lax.rem(lax.div(jnp.int32(code), t), 16)
            rows = pl.ds(pl.multiple_of(j * pad, pad), pad)
            cut = cap // 16 * 16
            for k in range(NE // 2):
                even, odd = xg[1, 2 * k, rows, :], xg[1, 2 * k + 1, rows, :]
                middle = jnp.concatenate(
                    [even[cut:].astype(F32)[:8], odd[:16].astype(F32)[8:]], axis=0
                ).astype(BF)
                o = 2 * cap * k
                srows[i, o : o + cut, :] = even[:cut]
                srows[i, o + cut : o + cut + 16, :] = middle
                srows[i, o + cut + 16 : o + 2 * cap, :] = odd[16:]
            spot = lax.broadcasted_iota(jnp.int32, (cap, T), 0).astype(F32)
            names = meta[i].astype(F32)[:8]
            out = jnp.zeros((8, T), F32)
            for e in range(NE):
                hit = spot == slots[i, e : e + 1, :]
                part = pl.ds(pl.multiple_of(j * pad + e % 2 * (pad - cap), 8), cap)
                val = jnp.sum(jnp.where(hit, sp[e, part, :][:, :1], 0.0), axis=0, keepdims=True)
                out = jnp.where(names == (ep * NE + e).astype(F32), val, out)
            ppg[i] = out
            return t * 16

        lax.fori_loop(0, count, finish, jnp.int32(1))

    lead = (("y", "z"), ("z", "y"))

    def source(h, da, db):
        return da * 4 + db if h == 0 else db * 4 + da

    def far(h, w, db):
        return copy(
            ("far", h, w, db), srows.at[source(h, 2, db), :, pl.ds(h * HD + w * QD, QD)],
            fr.at[h, w, db], nb[lead[h][0], w],
        )

    def nearc(h, w, db):
        return copy(
            ("nc", h, w, db), srows.at[source(h, 1 + 2 * w, db), :, pl.ds(h * HD + (1 - w) * QD, QD)],
            nc.at[h, w, db], nb[lead[h][0], w],
        )

    def nearm(h, w, db):
        return copy(("nm", h, w, db), pm.at[h, w, db], nm.at[h, w, db], nb[lead[h][0], w])

    def cols_of(c):
        return pl.ds(c * QD, QD)

    def far2(h, w, c):
        return copy(
            ("far2", h, w, c), q.at[h, 2, half[w], cols_of(c)], t1.at[h, w, :, cols_of(c)], nb[lead[h][1], w]
        )

    def near2(h, w, k, c):
        return copy(
            ("near2", h, w, k, c), q.at[h, 1 + 2 * w, half[k], cols_of(c)],
            gin.at[h, w, half[k], cols_of(c)], nb[lead[h][1], w],
        )

    issued = set()

    def issue_ready(b, dbs):
        for kind in ("far", "near"):
            for db in dbs:
                for h, w in both:
                    da = 2 if kind == "far" else 1 + 2 * w
                    if (kind, h, w, db) not in issued and DONE_IN[source(h, da, db)] <= b:
                        issued.add((kind, h, w, db))
                        start((far if kind == "far" else nearc)(h, w, db))

    def merge(db):
        for h, w in both:
            far(h, w, db).wait_recv()

        def add(n, _):
            h, w = lax.div(n, 2), lax.rem(n, 2)
            da = 1 + 2 * w
            i = (1 - h) * (da * 4 + db) + h * (db * 4 + da)
            cols = pl.ds(pl.multiple_of(h * HD + w * QD, QD), QD)
            lhs = jnp.concatenate([oh[i], oh[pair(h, 1 - w, 1, db)]], axis=0)
            rhs = jnp.concatenate([srows[i, :, cols], fr[h, w, db]], axis=0)
            pm[h, w, db] = dot_tn(lhs, rhs).astype(BF)
            return 0

        lax.fori_loop(0, 4, add, 0)
        for h, w in both:
            start(nearm(h, w, db))

    def total(db):
        for h, w in both:
            nearc(h, w, db).wait_recv()
            nearm(h, w, db).wait_recv()

        def add(n, _):
            h, k = lax.div(n, 2), lax.rem(n, 2)
            i = (1 - h) * db + h * (db * 4)
            cols = pl.ds(pl.multiple_of(h * HD + k * QD, QD), QD)
            lhs = jnp.concatenate([oh[i], oh[pair(h, k, 0, db)]], axis=0)
            rhs = jnp.concatenate([srows[i, :, cols], nc[h, 1 - k, db]], axis=0)
            res = dot_tn(lhs, rhs) + nm[h, k, db].astype(F32)
            part = pl.ds(pl.multiple_of(k * QD, QD), QD)
            if db == 0:
                facc[h, :, part] = res
            else:
                q[h, db, :, part] = res.astype(BF)
            return 0

        lax.fori_loop(0, 4, add, 0)

    weight_grads(0)
    for c in ms:
        c.wait_recv()
    prepare()
    send_c2(0)
    for p, w in both:
        p1(p, w, w).wait_recv()
        start(f1(p, w))
    for p, w in both:
        p1(p, w, 1 - w).wait_recv()
    send_p2(1)
    send_p2(3)
    send_c2(1)
    send_c2(3)
    weight_grads(1)
    relay(0)
    for c in weights:
        c.wait()
    wait_c2(0)
    batch(0)
    for p, w in both:
        f1(p, w).wait_recv()
    send_p2(2)
    send_c2(2)
    relay(1)
    relay(3)
    weight_grads(2)
    weight_grads(3)
    wait_r2(0)
    wait_c2(1)
    batch(1)
    wait_c2(3)
    batch(2)
    relay(2)
    issue_ready(2, (0, 1, 3, 2))
    wait_c2(2)
    wait_r2(1)
    batch(3)
    issue_ready(3, (1, 0, 3, 2))
    wait_r2(3)
    wait_r2(2)
    batch(4)
    issue_ready(4, (2, 3, 1, 0))
    merge(0)
    merge(1)
    merge(2)
    merge(3)
    pgs = [copy(("c", i), ppg.at[i], ppgr.at[mirror[i]], peers[i]) for i in range(1, 16)]
    for c in pgs:
        start(c)
    total(0)
    total(1)
    total(2)
    for c in range(2):
        for h, w in both:
            start(far2(h, w, c))
    total(3)
    for c in range(2):
        for h, w in both:
            start(near2(h, w, 1 - w, c))
        for h, w in both:
            far2(h, w, c).wait_recv()
            db = 1 + 2 * w
            q[h, db, half[w], cols_of(c)] = (
                q[h, db, half[w], cols_of(c)].astype(F32) + t1[h, w, :, cols_of(c)].astype(F32)
            ).astype(BF)
            start(near2(h, w, w, c))
    for c in pgs:
        c.wait_recv()
    routed = ppg[0]
    for i in range(1, 16):
        routed = routed + ppgr[i]
    pg_out[...] = routed
    ups = {}
    for c in range(2):
        for h in range(2):
            for w in range(2):
                for k in range(2):
                    near2(h, w, k, c).wait_recv()
            cols = pl.ds(h * HD + c * QD, QD)
            upv[:, cols] = (
                facc[h, :, cols_of(c)]
                + gin[h, 0, :, cols_of(c)].astype(F32)
                + gin[h, 1, :, cols_of(c)].astype(F32)
            ).astype(BF)
            ups[h, c] = copy(("up", h, c), upv.at[:, cols], up_out.at[:, cols], before)

            @pl.when(sec > 0)
            def _():
                ups[h, c].start()

    for c in sent:
        c.wait_send()
    for c in ups.values():
        @pl.when(sec > 0)
        def _():
            c.wait_send()

        @pl.when(sec < sections - 1)
        def _():
            c.wait_recv()


def deliver(up_in, pg_in, go_in, uo_in, up_out, pg_out, go_out, uo_out, sem):
    out = [(up_in, up_out)]
    for e in range(go_in.shape[0]):
        out += [(go_in.at[e], go_out.at[e]), (uo_in.at[e], uo_out.at[e])]
    out = [pltpu.make_async_copy(v, o, sem.at[k]) for k, (v, o) in enumerate(out)]
    for c in out:
        c.start()
    pg_out[...] = pg_in[...].astype(BF)
    for c in out:
        c.wait()


def per_device(sections, og, li, ids, probs, wg, wu, wd, si, sg, su, counts):
    T, D = og.shape[1], og.shape[2]
    NE, FF = wg.shape[1], wg.shape[3]
    SL = si.shape[2]
    cap = SL // 16
    pad = -(-cap // 16) * 16
    M, R = NE * cap, 4 * pad
    HD, QD, H = D // 2, D // 4, T // 2
    hbm = pl.BlockSpec(memory_space=pl.ANY)
    V = pltpu.VMEM
    up, pg, go, uo = pl.pallas_call(
        functools.partial(kernel, sections, cap, pad),
        out_shape=(
            V((T, D), BF),
            V((8, T), F32),
            V((NE, D, FF), BF),
            V((NE, D, FF), BF),
        ),
        in_specs=[hbm] * 2 + [pl.BlockSpec(memory_space=V)] * 2 + [hbm] * 6 + [pl.BlockSpec(memory_space=pltpu.SMEM)],
        out_specs=(pl.BlockSpec(memory_space=V),) * 4,
        scratch_shapes=[
            V((2, 16, T, HD), BF), V((2, 16, M, HD), BF), V((2, 2, 4, M, HD), BF), V((2, 2, 4, M, HD), BF),
            V((16, 16, T), BF), V((NE, D, 2 * FF), BF), V((NE, FF, D), BF),
            V((SL, D), BF), V((2, SL, FF), BF), V((SL, 2 * FF), BF),
            V((48, 8, T), F32), V((48, 8, T), F32), V((T, T), BF), V((48, M, T), BF),
            V((2, NE, R, D), BF), V((NE, R, 128), F32), V((NE, R, 128), F32), V((16, M, D), BF),
            V((2, 2, 4, M, QD), BF), V((2, 2, 4, M, QD), BF),
            V((2, 2, 4, T, QD), BF), V((2, 2, 4, T, QD), BF),
            V((2, 4, T, HD), BF), V((2, 2, H, HD), BF), V((2, 2, T, HD), BF), V((2, T, HD), F32),
            V((T, D), BF), V((16, 8, T), F32), V((16, 8, T), F32),
            pltpu.SemaphoreType.DMA((N_SEMS,)), pltpu.SemaphoreType.DMA((N_SEMS,)),
            pltpu.SemaphoreType.DMA((14,)),
        ],
        compiler_params=pltpu.CompilerParams(
            collective_id=0, has_side_effects=True, vmem_limit_bytes=59_800_000
        ),
    )(og[0], li[0], ids[0].T, probs[0].T, wg[0], wu[0], wd[0], si[0], sg[0], su[0], counts[0])
    up, pg, go, uo = pl.pallas_call(
        deliver,
        out_shape=(
            jax.ShapeDtypeStruct((T, D), BF),
            jax.ShapeDtypeStruct((8, T), BF),
            jax.ShapeDtypeStruct((NE, D, FF), BF),
            jax.ShapeDtypeStruct((NE, D, FF), BF),
        ),
        in_specs=[pl.BlockSpec(memory_space=V)] * 4,
        out_specs=(hbm, pl.BlockSpec(memory_space=V), hbm, hbm),
        scratch_shapes=[pltpu.SemaphoreType.DMA((1 + 2 * NE,))],
        compiler_params=pltpu.CompilerParams(vmem_limit_bytes=16 * 2**20),
    )(up, pg, go, uo)
    return up[None], pg.T[None], go[None], uo[None]


def solution(mesh):
    return jax.shard_map(
        functools.partial(per_device, mesh.shape["section"]),
        mesh=mesh,
        in_specs=(
            P("section", "ep", None),
            P("section", "ep", None),
            P("section", "ep", None),
            P("section", "ep", None),
            P("section", "ep", None, None),
            P("section", "ep", None, None),
            P("section", "ep", None, None),
            P("section", "ep", None, None),
            P("section", "ep", None, None),
            P("section", "ep", None, None),
            P("section", "ep", None),
        ),
        out_specs=(
            P("section", "ep", None),
            P("section", "ep", None),
            P("section", "ep", None, None),
            P("section", "ep", None, None),
        ),
        check_vma=False,
    )
```

```python
import functools

import jax
import jax.numpy as jnp
from jax import lax
from jax.experimental import pallas as pl
from jax.experimental.pallas import tpu as pltpu
from jax.sharding import PartitionSpec as P

MESH = pl.DeviceIdType.MESH
BF = jnp.bfloat16
F32 = jnp.float32

RAW = ((0, 0), (0, 1), (1, 0), (0, 2), (2, 0), (2, 3))
RAW_PARENT = (None, 0, 0, 1, 2, 4)
LEAF = ((0, 3), (3, 0), (1, 1), (3, 1), (1, 3), (1, 2), (3, 2), (2, 1), (2, 2), (3, 3))
LEAF_PARENT = (0, 0, 1, 1, 2, 3, 3, 4, 5, 5)
NL = len(LEAF)
IMAGES = range(4)
BATCHES = ((0, 1, 3, 4, 12), (7, 13, 2, 8), (5, 15, 10), (6, 14, 9, 11))
PAIRS = 16 + 4 * NL
N_SEMS = 224
CHUNKS = 2


def image(v, node):
    dy, dz = node if v < 2 else node[::-1]
    return ((-dy) % 4, (-dz) % 4) if v % 2 else (dy, dz)


def image_at(v, node):
    swap, flip = lax.div(v, 2), lax.rem(v, 2)
    dy = (1 - swap) * node[0] + swap * node[1]
    dz = (1 - swap) * node[1] + swap * node[0]
    return lax.rem((1 - flip) * dy + flip * (4 - dy), 4), lax.rem((1 - flip) * dz + flip * (4 - dz), 4)


def minus(node):
    return (-node[0]) % 4, (-node[1]) % 4


def step(parent, child):
    return (child[0] - parent[0]) % 4, (child[1] - parent[1]) % 4


def dot(a, b):
    return jnp.dot(a, b, preferred_element_type=F32)


def dot_nt(a, b):
    return lax.dot_general(a, b, (((1,), (1,)), ((), ())), preferred_element_type=F32)


def dot_tn(a, b):
    return lax.dot_general(a, b, (((0,), (0,)), ((), ())), preferred_element_type=F32)


def kernel(
    sections, cap, pad,
    g_in, x_in, ids_in, prob_in, wg_in, wu_in, wd_in, si_in, sg_in, su_in, cnt,
    up_out, pg_out, go_out, uo_out,
    raw, cmp, sendc, meta, wgu, wd,
    si, sgu_raw, sgu,
    memb, slots, upper, oh, xg, pv, sp, srows,
    fr, pm, nm, upv, ppg, ppgr,
    ssem, rsem, lsem,
):
    T, HD = raw.shape[2], raw.shape[3]
    D = 2 * HD
    NE, FF = wd.shape[0], wd.shape[1]
    SL = si.shape[0]
    QD = HD // 2
    M = NE * cap
    TC = T // CHUNKS
    sec = lax.axis_index("section")
    ep = lax.axis_index("ep")
    y, z = lax.div(ep, 4), lax.rem(ep, 4)

    def at(yy, zz):
        return {"ep": lax.rem(yy, 4) * 4 + lax.rem(zz, 4)}

    peers = {i: at(y + i // 4, z + i % 4) for i in range(1, 16)}
    mirror = {i: (4 - i // 4) % 4 * 4 + (4 - i % 4) % 4 for i in range(1, 16)}
    before = {"section": lax.rem(sec + sections - 1, sections)}
    after = {"section": lax.rem(sec + 1, sections)}

    ids = {}
    sent = []

    def copy(key, src, dst, dev):
        k = ids.setdefault(key, len(ids))
        return pltpu.make_async_remote_copy(
            src_ref=src, dst_ref=dst, send_sem=ssem.at[k], recv_sem=rsem.at[k],
            device_id=dev, device_id_type=MESH,
        )

    def start(c):
        c.start()
        sent.append(c)

    def load(k, src, dst):
        return pltpu.make_async_copy(src, dst, lsem.at[k])

    own = [
        load(1 + 2 * p + ch, ref.at[:, pl.ds(ch * HD, HD)], raw.at[2 * p + ch, 0])
        for p, ref in enumerate((g_in, x_in)) for ch in range(2)
    ]
    for c in own:
        c.start()
    weights = [
        load(5, wg_in, wgu.at[:, :, pl.ds(0, FF)]),
        load(6, wu_in, wgu.at[:, :, pl.ds(FF, FF)]),
        load(7, wd_in, wd),
    ]

    def saved(e):
        return [
            load(8, si_in.at[e], si),
            load(9, sg_in.at[e], sgu_raw.at[0]),
            load(10, su_in.at[e], sgu_raw.at[1]),
        ]

    barrier = pltpu.get_barrier_semaphore()
    for dev in (*peers.values(), before, after):
        pl.semaphore_signal(barrier, inc=1, device_id=dev, device_id_type=MESH)
    for c in saved(0):
        c.start()
    for c in weights:
        c.start()
    meta[0] = jnp.concatenate([ids_in[...].astype(F32), prob_in[...].astype(F32)], axis=0).astype(BF)
    pl.semaphore_wait(barrier, 17)
    for c in own:
        c.wait()

    def toward(v, parent, child):
        dy, dz = image(v, step(parent, child))
        return at(y + dy, z + dz)

    def source(v, node):
        dy, dz = image(v, minus(node))
        return dy * 4 + dz

    def source_at(v, node):
        dy, dz = image_at(v, minus(node))
        return dy * 4 + dz

    def raw_down(v, k):
        r = RAW_PARENT[k]
        return copy(("raw", v, k), raw.at[v, r], raw.at[v, k], toward(v, RAW[r], RAW[k]))

    def leaf_down(v, l):
        return copy(("leaf", v, l), sendc.at[v, l], cmp.at[v, l], toward(v, RAW[LEAF_PARENT[l]], LEAF[l]))

    def send_leaf(*ls):
        for l in ls:
            def pick(v, _):
                sendc[v, l] = dot(oh[16 + v * NL + l], raw[v, LEAF_PARENT[l]]).astype(BF)
                return 0

            lax.fori_loop(0, 4, pick, 0)
            for v in IMAGES:
                start(leaf_down(v, l))

    def wait_raw(*ks):
        for k in ks:
            for v in IMAGES:
                raw_down(v, k).wait_recv()

    def wait_leaf(*ls):
        for l in ls:
            for v in IMAGES:
                leaf_down(v, l).wait_recv()

    def pass_raw(k, child):
        for v in IMAGES:
            raw_down(v, k).wait_recv()
            start(raw_down(v, child))

    ms = [copy(("m", i), meta.at[0], meta.at[mirror[i]], peers[i]) for i in range(1, 16)]
    for c in ms:
        start(c)
    for k in (1, 2):
        for v in IMAGES:
            start(raw_down(v, k))

    @pl.when(sec == sections - 1)
    def _():
        up_out[...] = jnp.zeros(up_out.shape, BF)

    upper[...] = jnp.where(
        lax.broadcasted_iota(jnp.int32, (T, T), 0) < lax.broadcasted_iota(jnp.int32, (T, T), 1), 1.0, 0.0
    ).astype(BF)
    pv[...] = jnp.zeros(pv.shape, F32)

    def weight_grads(e):
        for c in saved(e):
            c.wait()
        row = lax.broadcasted_iota(jnp.int32, (SL, 1), 0)
        live = jnp.zeros((SL, 1), F32)
        for s in range(SL // cap):
            inside = (row >= s * cap) & (row < s * cap + cnt[e, s])
            live = jnp.where(inside, 1.0, live)
        for k in range(2):
            sgu[:, pl.ds(k * FF, FF)] = (sgu_raw[k].astype(F32) * live).astype(BF)
        width = min(256, D)

        def chunk(c, _):
            cols = pl.ds(pl.multiple_of(c * width, width), width)
            res = dot_tn(si[:, cols], sgu[...]).astype(BF)
            go_out[e, cols, :] = res[:, :FF]
            uo_out[e, cols, :] = res[:, FF:]
            return 0

        lax.fori_loop(0, D // width, chunk, 0)
        if e + 1 < NE:
            for c in saved(e + 1):
                c.start()

    def member(n, i, owner):
        m = meta[i].astype(F32)
        names, probs = m[:8], m[8:]
        row = lax.broadcasted_iota(jnp.int32, (8, T), 0)
        is_in = jnp.zeros((8, T), F32)
        prob = jnp.zeros((8, T), F32)
        for e in range(NE):
            here = names == (owner * NE + e).astype(F32)
            me = jnp.max(jnp.where(here, 1.0, 0.0), axis=0, keepdims=True)
            pe = jnp.sum(jnp.where(here, probs, 0.0), axis=0, keepdims=True)
            is_in = jnp.where(row == e, me, is_in)
            prob = jnp.where(row == e + 4, pe, prob)
        memb[n] = is_in
        slots[n] = prob

    def member_self(n, _):
        member(n, n, ep)
        return 0

    def member_near(l):
        parent = RAW[LEAF_PARENT[l]]

        def member_of(v, _):
            dy, dz = image_at(v, step(parent, LEAF[l]))
            owner = lax.rem(y + dy, 4) * 4 + lax.rem(z + dz, 4)
            member(16 + v * NL + l, source_at(v, parent), owner)
            return 0

        lax.fori_loop(0, 4, member_of, 0)

    def one_hot(n, _):
        spot = lax.broadcasted_iota(jnp.int32, (cap, T), 0).astype(F32)
        rows = [jnp.where(spot == slots[n, e : e + 1, :], 1.0, 0.0) for e in range(NE)]
        oh[n] = jnp.concatenate(rows, axis=0).astype(BF)
        return 0

    def prepare():
        lax.fori_loop(0, 16, member_self, 0)
        for l in range(NL):
            member_near(l)
        inside = memb[...].reshape(PAIRS * 8, T)
        rank = dot(inside.astype(BF), upper[...])
        row = lax.rem(lax.broadcasted_iota(jnp.int32, (PAIRS * 8, T), 0), 8)
        prob = slots[...].reshape(PAIRS * 8, T)
        slots[...] = jnp.where(row < 4, jnp.where(inside > 0.5, rank, -1.0), prob).reshape(PAIRS, 8, T)
        lax.fori_loop(0, PAIRS, one_hot, 0)

    def dispatch(b, node):
        slot = sum(BATCHES[b].index(source(v, node)) * 8**v for v in IMAGES)

        def bring(v, t):
            j = lax.rem(lax.div(jnp.int32(slot), t), 8)
            p, ch = lax.div(v, 2), lax.rem(v, 2)
            if node in RAW:
                piece = dot(oh[source_at(v, node)], raw[v, RAW.index(node)]).astype(BF)
            else:
                piece = cmp[v, LEAF.index(node)]
            rows = pl.ds(pl.multiple_of(j * pad, pad), pad)
            cols = pl.ds(pl.multiple_of(ch * HD, HD), HD)
            for k in range(NE // 2):
                xg[p, 2 * k, rows, cols] = piece[2 * cap * k : 2 * cap * k + pad]
                xg[p, 2 * k + 1, rows, cols] = piece[2 * cap * (k + 1) - pad : 2 * cap * (k + 1)]
            return t * 8

        lax.fori_loop(0, 4, bring, jnp.int32(1))

    def batch(b):
        code = sum(i * 16**j for j, i in enumerate(BATCHES[b]))
        count = len(BATCHES[b])
        used = pl.ds(0, count * pad)
        for i in BATCHES[b]:
            dispatch(b, (i // 4, i % 4))

        def weigh(j, t):
            i = lax.rem(lax.div(jnp.int32(code), t), 16)
            spot = lax.broadcasted_iota(jnp.int32, (cap, T), 0).astype(F32)
            for e in range(NE):
                hit = spot == slots[i, e : e + 1, :]
                weight = jnp.sum(
                    jnp.where(hit, slots[i, e + 4 : e + 5, :], 0.0), axis=1, keepdims=True
                )
                rows = pl.ds(pl.multiple_of(j * pad + e % 2 * (pad - cap), 8), cap)
                pv[e, rows, :] = jnp.broadcast_to(weight, (cap, 128))
            return t * 16

        lax.fori_loop(0, count, weigh, jnp.int32(1))

        def expert(e, _):
            gate_up = dot(xg[1, e, used, :], wgu[e])
            gate, up = gate_up[:, :FF], gate_up[:, FF:]
            hg = dot_nt(xg[0, e, used, :], wd[e])
            sigma = jax.nn.sigmoid(gate)
            active = gate * sigma
            hidden = (active * up).astype(BF).astype(F32)
            slot_prob = jnp.sum(hidden * hg, axis=1, keepdims=True)
            sp[e, used, :] = jnp.broadcast_to(slot_prob, (count * pad, 128))
            scaled = hg * pv[e, used, :][:, :1]
            gg = (scaled * up * sigma * (1.0 + gate * (1.0 - sigma))).astype(BF)
            ug = (scaled * active).astype(BF)
            xg[1, e, used, :] = dot_nt(jnp.concatenate([gg, ug], axis=1), wgu[e]).astype(BF)
            return 0

        lax.fori_loop(0, NE, expert, 0)

        def finish(j, t):
            i = lax.rem(lax.div(jnp.int32(code), t), 16)
            rows = pl.ds(pl.multiple_of(j * pad, pad), pad)
            cut = cap // 16 * 16
            for k in range(NE // 2):
                even, odd = xg[1, 2 * k, rows, :], xg[1, 2 * k + 1, rows, :]
                middle = jnp.concatenate(
                    [even[cut:].astype(F32)[:8], odd[:16].astype(F32)[8:]], axis=0
                ).astype(BF)
                o = 2 * cap * k
                srows[i, o : o + cut, :] = even[:cut]
                srows[i, o + cut : o + cut + 16, :] = middle
                srows[i, o + cut + 16 : o + 2 * cap, :] = odd[16:]
            spot = lax.broadcasted_iota(jnp.int32, (cap, T), 0).astype(F32)
            names = meta[i].astype(F32)[:8]
            out = jnp.zeros((8, T), F32)
            for e in range(NE):
                hit = spot == slots[i, e : e + 1, :]
                part = pl.ds(pl.multiple_of(j * pad + e % 2 * (pad - cap), 8), cap)
                val = jnp.sum(jnp.where(hit, sp[e, part, :][:, :1], 0.0), axis=0, keepdims=True)
                out = jnp.where(names == (ep * NE + e).astype(F32), val, out)
            ppg[i] = out.astype(BF)
            return t * 16

        lax.fori_loop(0, count, finish, jnp.int32(1))

    def leaf_up(v, l):
        return copy(
            ("up_leaf", v, l), srows.at[source(v, LEAF[l]), :, pl.ds(v * QD, QD)], fr.at[v, l],
            toward(v, LEAF[l], RAW[LEAF_PARENT[l]]),
        )

    def raw_up(v, k, c):
        rows = pl.ds(c * TC, TC)
        return copy(
            ("up_raw", v, k, c), pm.at[v, k - 1, rows], nm.at[v, k - 1, rows],
            toward(v, RAW[k], RAW[RAW_PARENT[k]]),
        )

    def return_leaf(*ls):
        for l in ls:
            for v in IMAGES:
                start(leaf_up(v, l))

    def children(k):
        return [l for l in range(NL) if LEAF_PARENT[l] == k], [c for c in range(1, len(RAW)) if RAW_PARENT[c] == k]

    def gathered(k, c, v, i, cols):
        leaves, raws = children(k)
        rows = pl.ds(c * TC, TC)
        lhs = jnp.concatenate([oh[i, :, rows]] + [oh[16 + v * NL + l, :, rows] for l in leaves], axis=0)
        rhs = jnp.concatenate([srows[i, :, cols]] + [fr[v, l] for l in leaves], axis=0)
        res = dot_tn(lhs, rhs)
        for r in raws:
            res = res + nm[v, r - 1, rows, :].astype(F32)
        return res

    def wait_children(k, c, v):
        leaves, raws = children(k)
        if c == 0:
            for l in leaves:
                leaf_up(v, l).wait_recv()
        for r in raws:
            raw_up(v, r, c).wait_recv()

    def merge(k, c):
        for v in IMAGES:
            wait_children(k, c, v)

        def add(v, _):
            cols = pl.ds(pl.multiple_of(v * QD, QD), QD)
            pm[v, k - 1, pl.ds(c * TC, TC), :] = gathered(k, c, v, source_at(v, RAW[k]), cols).astype(BF)
            return 0

        lax.fori_loop(0, 4, add, 0)
        for v in IMAGES:
            start(raw_up(v, k, c))

    weight_grads(0)
    for c in ms:
        c.wait_recv()
    prepare()
    send_leaf(0, 1)
    pass_raw(1, 3)
    pass_raw(2, 4)
    send_leaf(3)
    weight_grads(1)
    for c in weights:
        c.wait()
    wait_leaf(0, 1)
    batch(0)
    wait_raw(3)
    pass_raw(4, 5)
    send_leaf(4, 2)
    weight_grads(2)
    wait_raw(5)
    send_leaf(8, 9)
    send_leaf(5, 6, 7)
    wait_leaf(3, 4)
    batch(1)
    return_leaf(3, 4)
    weight_grads(3)
    wait_leaf(2, 8, 9)
    batch(2)
    return_leaf(8, 9, 2)
    wait_leaf(5, 6, 7)
    batch(3)
    return_leaf(5, 6)
    merge(5, 0)
    merge(5, 1)
    return_leaf(7)
    merge(3, 0)
    merge(3, 1)
    return_leaf(0, 1)
    merge(4, 0)
    merge(1, 0)
    merge(4, 1)
    merge(2, 0)
    merge(1, 1)
    pgs = [copy(("c", i), ppg.at[i], ppgr.at[mirror[i]], peers[i]) for i in range(1, 16)]
    for c in pgs:
        start(c)
    merge(2, 1)
    ups = {}
    for c in range(CHUNKS):
        for v in IMAGES:
            rows, cols = pl.ds(c * TC, TC), pl.ds(v * QD, QD)
            wait_children(0, c, v)
            upv[rows, cols] = gathered(0, c, v, 0, cols).astype(BF)
            ups[v, c] = copy(("up", v, c), upv.at[rows, cols], up_out.at[rows, cols], before)

            @pl.when(sec > 0)
            def _():
                ups[v, c].start()

    for c in pgs:
        c.wait_recv()
    routed = ppg[0].astype(F32)
    for i in range(1, 16):
        routed = routed + ppgr[i].astype(F32)
    pg_out[...] = routed

    for c in sent:
        c.wait_send()
    for c in ups.values():
        @pl.when(sec > 0)
        def _():
            c.wait_send()

        @pl.when(sec < sections - 1)
        def _():
            c.wait_recv()


def deliver(up_in, pg_in, go_in, uo_in, up_out, pg_out, go_out, uo_out, sem):
    out = [(up_in, up_out)]
    for e in range(go_in.shape[0]):
        out += [(go_in.at[e], go_out.at[e]), (uo_in.at[e], uo_out.at[e])]
    out = [pltpu.make_async_copy(v, o, sem.at[k]) for k, (v, o) in enumerate(out)]
    for c in out:
        c.start()
    pg_out[...] = pg_in[...].astype(BF)
    for c in out:
        c.wait()


def per_device(sections, og, li, ids, probs, wg, wu, wd, si, sg, su, counts):
    T, D = og.shape[1], og.shape[2]
    NE, FF = wg.shape[1], wg.shape[3]
    SL = si.shape[2]
    cap = SL // 16
    pad = -(-cap // 16) * 16
    M, R = NE * cap, max(map(len, BATCHES)) * pad
    HD, QD = D // 2, D // 4
    hbm = pl.BlockSpec(memory_space=pl.ANY)
    V = pltpu.VMEM
    up, pg, go, uo = pl.pallas_call(
        functools.partial(kernel, sections, cap, pad),
        out_shape=(
            V((T, D), BF),
            V((8, T), F32),
            V((NE, D, FF), BF),
            V((NE, D, FF), BF),
        ),
        in_specs=[hbm] * 2 + [pl.BlockSpec(memory_space=V)] * 2 + [hbm] * 6 + [pl.BlockSpec(memory_space=pltpu.SMEM)],
        out_specs=(pl.BlockSpec(memory_space=V),) * 4,
        scratch_shapes=[
            V((4, len(RAW), T, HD), BF), V((4, NL, M, HD), BF), V((4, NL, M, HD), BF),
            V((16, 16, T), BF), V((NE, D, 2 * FF), BF), V((NE, FF, D), BF),
            V((SL, D), BF), V((2, SL, FF), BF), V((SL, 2 * FF), BF),
            V((PAIRS, 8, T), F32), V((PAIRS, 8, T), F32), V((T, T), BF), V((PAIRS, M, T), BF),
            V((2, NE, R, D), BF), V((NE, R, 128), F32), V((NE, R, 128), F32), V((16, M, D), BF),
            V((4, NL, M, QD), BF), V((4, len(RAW) - 1, T, QD), BF), V((4, len(RAW) - 1, T, QD), BF),
            V((T, D), BF), V((16, 8, T), BF), V((16, 8, T), BF),
            pltpu.SemaphoreType.DMA((N_SEMS,)), pltpu.SemaphoreType.DMA((N_SEMS,)),
            pltpu.SemaphoreType.DMA((14,)),
        ],
        compiler_params=pltpu.CompilerParams(
            collective_id=0, has_side_effects=True, vmem_limit_bytes=59_800_000
        ),
    )(og[0], li[0], ids[0].T, probs[0].T, wg[0], wu[0], wd[0], si[0], sg[0], su[0], counts[0])
    up, pg, go, uo = pl.pallas_call(
        deliver,
        out_shape=(
            jax.ShapeDtypeStruct((T, D), BF),
            jax.ShapeDtypeStruct((8, T), BF),
            jax.ShapeDtypeStruct((NE, D, FF), BF),
            jax.ShapeDtypeStruct((NE, D, FF), BF),
        ),
        in_specs=[pl.BlockSpec(memory_space=V)] * 4,
        out_specs=(hbm, pl.BlockSpec(memory_space=V), hbm, hbm),
        scratch_shapes=[pltpu.SemaphoreType.DMA((1 + 2 * NE,))],
        compiler_params=pltpu.CompilerParams(vmem_limit_bytes=16 * 2**20),
    )(up, pg, go, uo)
    return up[None], pg.T[None], go[None], uo[None]


def solution(mesh):
    return jax.shard_map(
        functools.partial(per_device, mesh.shape["section"]),
        mesh=mesh,
        in_specs=(
            P("section", "ep", None),
            P("section", "ep", None),
            P("section", "ep", None),
            P("section", "ep", None),
            P("section", "ep", None, None),
            P("section", "ep", None, None),
            P("section", "ep", None, None),
            P("section", "ep", None, None),
            P("section", "ep", None, None),
            P("section", "ep", None, None),
            P("section", "ep", None),
        ),
        out_specs=(
            P("section", "ep", None),
            P("section", "ep", None),
            P("section", "ep", None, None),
            P("section", "ep", None, None),
        ),
        check_vma=False,
    )
```

```python
import functools

import jax
import jax.numpy as jnp
from jax import lax
from jax.experimental import pallas as pl
from jax.experimental.pallas import tpu as pltpu
from jax.sharding import PartitionSpec as P

MESH = pl.DeviceIdType.MESH
BF = jnp.bfloat16
F32 = jnp.float32

RAW = ((0, 0), (0, 1), (1, 0), (0, 2), (2, 0), (2, 3))
RAW_PARENT = (None, 0, 0, 1, 2, 4)
LEAF = ((0, 3), (3, 0), (1, 1), (3, 1), (1, 3), (1, 2), (3, 2), (2, 1), (2, 2), (3, 3))
LEAF_PARENT = (0, 0, 1, 1, 2, 3, 3, 4, 5, 5)
NL = len(LEAF)
IMAGES = range(4)
BATCHES = ((0, 1, 3, 4, 12), (7, 13, 2, 8), (5, 15, 10), (6, 14, 9, 11))
PAIRS = 16 + 4 * NL
N_SEMS = 224
CHUNKS = 2


def image(v, node):
    dy, dz = node if v < 2 else node[::-1]
    return ((-dy) % 4, (-dz) % 4) if v % 2 else (dy, dz)


def image_at(v, node):
    swap, flip = lax.div(v, 2), lax.rem(v, 2)
    dy = (1 - swap) * node[0] + swap * node[1]
    dz = (1 - swap) * node[1] + swap * node[0]
    return lax.rem((1 - flip) * dy + flip * (4 - dy), 4), lax.rem((1 - flip) * dz + flip * (4 - dz), 4)


def minus(node):
    return (-node[0]) % 4, (-node[1]) % 4


def parent_of(node):
    return RAW[RAW_PARENT[RAW.index(node)] if node in RAW else LEAF_PARENT[LEAF.index(node)]]


def step(parent, child):
    return (child[0] - parent[0]) % 4, (child[1] - parent[1]) % 4


def dot(a, b):
    return jnp.dot(a, b, preferred_element_type=F32)


def dot_nt(a, b):
    return lax.dot_general(a, b, (((1,), (1,)), ((), ())), preferred_element_type=F32)


def dot_tn(a, b):
    return lax.dot_general(a, b, (((0,), (0,)), ((), ())), preferred_element_type=F32)


def kernel(
    sections, cap, pad,
    g_in, x_in, ids_in, prob_in, wg_in, wu_in, wd_in, si_in, sg_in, su_in, cnt,
    up_out, pg_out, go_out, uo_out,
    raw, cmp, sendc, meta, wgu, wd,
    si, sgu_raw, sgu,
    memb, slots, upper, oh, xg, pv, sp, srows,
    fr, pm, nm, upv, ppg, ppgr,
    ssem, rsem, lsem,
):
    T, HD = raw.shape[2], raw.shape[3]
    D = 2 * HD
    NE, FF = wd.shape[0], wd.shape[1]
    SL = si.shape[0]
    QD = HD // 2
    M = NE * cap
    TC = T // CHUNKS
    sec = lax.axis_index("section")
    ep = lax.axis_index("ep")
    y, z = lax.div(ep, 4), lax.rem(ep, 4)

    def at(yy, zz):
        return {"ep": lax.rem(yy, 4) * 4 + lax.rem(zz, 4)}

    before = {"section": lax.rem(sec + sections - 1, sections)}
    after = {"section": lax.rem(sec + 1, sections)}

    ids = {}
    sent = []

    def copy(key, src, dst, dev):
        k = ids.setdefault(key, len(ids))
        return pltpu.make_async_remote_copy(
            src_ref=src, dst_ref=dst, send_sem=ssem.at[k], recv_sem=rsem.at[k],
            device_id=dev, device_id_type=MESH,
        )

    def start(c):
        c.start()
        sent.append(c)

    def load(k, src, dst):
        return pltpu.make_async_copy(src, dst, lsem.at[k])

    own = [
        load(1 + 2 * p + ch, ref.at[:, pl.ds(ch * HD, HD)], raw.at[2 * p + ch, 0])
        for p, ref in enumerate((g_in, x_in)) for ch in range(2)
    ]
    for c in own:
        c.start()
    weights = [
        load(5, wg_in, wgu.at[:, :, pl.ds(0, FF)]),
        load(6, wu_in, wgu.at[:, :, pl.ds(FF, FF)]),
        load(7, wd_in, wd),
    ]

    def saved(e):
        return [
            load(8, si_in.at[e], si),
            load(9, sg_in.at[e], sgu_raw.at[0]),
            load(10, su_in.at[e], sgu_raw.at[1]),
        ]

    barrier = pltpu.get_barrier_semaphore()
    for dev in (at(y + 1, z), at(y + 3, z), at(y, z + 1), at(y, z + 3), before, after):
        pl.semaphore_signal(barrier, inc=1, device_id=dev, device_id_type=MESH)
    for c in saved(0):
        c.start()
    for c in weights:
        c.start()
    meta[0] = jnp.concatenate([ids_in[...].astype(F32), prob_in[...].astype(F32)], axis=0).astype(BF)
    memb[...] = jnp.zeros(memb.shape, F32)
    slots[...] = jnp.zeros(slots.shape, F32)
    pl.semaphore_wait(barrier, 6)
    for c in own:
        c.wait()

    def toward(v, parent, child):
        dy, dz = image(v, step(parent, child))
        return at(y + dy, z + dz)

    def source(v, node):
        dy, dz = image(v, minus(node))
        return dy * 4 + dz

    def source_at(v, node):
        dy, dz = image_at(v, minus(node))
        return dy * 4 + dz

    def raw_down(v, k):
        r = RAW_PARENT[k]
        return copy(("raw", v, k), raw.at[v, r], raw.at[v, k], toward(v, RAW[r], RAW[k]))

    def leaf_down(v, l):
        return copy(("leaf", v, l), sendc.at[v, l], cmp.at[v, l], toward(v, RAW[LEAF_PARENT[l]], LEAF[l]))

    def send_leaf(*ls):
        for l in ls:
            def pick(v, _):
                sendc[v, l] = dot(oh[16 + 4 * l + v], raw[v, LEAF_PARENT[l]]).astype(BF)
                return 0

            lax.fori_loop(0, 4, pick, 0)
            for v in IMAGES:
                start(leaf_down(v, l))

    def wait_raw(*ks):
        for k in ks:
            for v in IMAGES:
                raw_down(v, k).wait_recv()

    def wait_leaf(*ls):
        for l in ls:
            for v in IMAGES:
                leaf_down(v, l).wait_recv()

    def pass_raw(k, child):
        for v in IMAGES:
            raw_down(v, k).wait_recv()
            start(raw_down(v, child))

    def meta_down(node):
        parent = parent_of(node)
        return copy(
            ("meta", node), meta.at[source(0, parent)], meta.at[source(0, node)], toward(0, parent, node)
        )

    def send_meta(*nodes):
        for node in nodes:
            start(meta_down(node))

    def wait_meta(*nodes):
        for node in nodes:
            meta_down(node).wait_recv()

    def send_raw(k):
        for v in IMAGES:
            start(raw_down(v, k))

    send_meta((0, 1), (1, 0), (0, 3), (3, 0))

    def clear():
        @pl.when(sec == sections - 1)
        def _():
            up_out[...] = jnp.zeros(up_out.shape, BF)

        upper[...] = jnp.where(
            lax.broadcasted_iota(jnp.int32, (T, T), 0) < lax.broadcasted_iota(jnp.int32, (T, T), 1), 1.0, 0.0
        ).astype(BF)
        pv[...] = jnp.zeros(pv.shape, F32)

    def weight_grads(e):
        for c in saved(e):
            c.wait()
        row = lax.broadcasted_iota(jnp.int32, (SL, 1), 0)
        live = jnp.zeros((SL, 1), F32)
        for s in range(SL // cap):
            inside = (row >= s * cap) & (row < s * cap + cnt[e, s])
            live = jnp.where(inside, 1.0, live)
        for k in range(2):
            sgu[:, pl.ds(k * FF, FF)] = (sgu_raw[k].astype(F32) * live).astype(BF)
        width = min(256, D)

        def chunk(c, _):
            cols = pl.ds(pl.multiple_of(c * width, width), width)
            res = dot_tn(si[:, cols], sgu[...]).astype(BF)
            go_out[e, cols, :] = res[:, :FF]
            uo_out[e, cols, :] = res[:, FF:]
            return 0

        lax.fori_loop(0, D // width, chunk, 0)
        if e + 1 < NE:
            for c in saved(e + 1):
                c.start()

    def member(n, i, owner):
        m = meta[i].astype(F32)
        names, probs = m[:8], m[8:]
        row = lax.broadcasted_iota(jnp.int32, (8, T), 0)
        is_in = jnp.zeros((8, T), F32)
        prob = jnp.zeros((8, T), F32)
        for e in range(NE):
            here = names == (owner * NE + e).astype(F32)
            me = jnp.max(jnp.where(here, 1.0, 0.0), axis=0, keepdims=True)
            pe = jnp.sum(jnp.where(here, probs, 0.0), axis=0, keepdims=True)
            is_in = jnp.where(row == e, me, is_in)
            prob = jnp.where(row == e + 4, pe, prob)
        memb[n] = is_in
        slots[n] = prob

    def member_near(l):
        parent = RAW[LEAF_PARENT[l]]

        def member_of(v, _):
            dy, dz = image_at(v, step(parent, LEAF[l]))
            owner = lax.rem(y + dy, 4) * 4 + lax.rem(z + dz, 4)
            member(16 + 4 * l + v, source_at(v, parent), owner)
            return 0

        lax.fori_loop(0, 4, member_of, 0)

    def one_hot(n, _):
        spot = lax.broadcasted_iota(jnp.int32, (cap, T), 0).astype(F32)
        rows = [jnp.where(spot == slots[n, e : e + 1, :], 1.0, 0.0) for e in range(NE)]
        oh[n] = jnp.concatenate(rows, axis=0).astype(BF)
        return 0

    def prepare(sources, leaves):
        for i in sources:
            member(i, i, ep)
        for l in leaves:
            member_near(l)
        inside = memb[...].reshape(PAIRS * 8, T)
        rank = dot(inside.astype(BF), upper[...])
        row = lax.rem(lax.broadcasted_iota(jnp.int32, (PAIRS * 8, T), 0), 8)
        prob = slots[...].reshape(PAIRS * 8, T)
        slots[...] = jnp.where(row < 4, jnp.where(inside > 0.5, rank, -1.0), prob).reshape(PAIRS, 8, T)
        for i in sources:
            one_hot(i, 0)
        if leaves:
            lax.fori_loop(16 + 4 * leaves[0], 20 + 4 * leaves[-1], one_hot, 0)

    def dispatch(b, node):
        slot = sum(BATCHES[b].index(source(v, node)) * 8**v for v in IMAGES)

        def bring(v, t):
            j = lax.rem(lax.div(jnp.int32(slot), t), 8)
            p, ch = lax.div(v, 2), lax.rem(v, 2)
            if node in RAW:
                piece = dot(oh[source_at(v, node)], raw[v, RAW.index(node)]).astype(BF)
            else:
                piece = cmp[v, LEAF.index(node)]
            rows = pl.ds(pl.multiple_of(j * pad, pad), pad)
            cols = pl.ds(pl.multiple_of(ch * HD, HD), HD)
            for k in range(NE // 2):
                xg[p, 2 * k, rows, cols] = piece[2 * cap * k : 2 * cap * k + pad]
                xg[p, 2 * k + 1, rows, cols] = piece[2 * cap * (k + 1) - pad : 2 * cap * (k + 1)]
            return t * 8

        lax.fori_loop(0, 4, bring, jnp.int32(1))

    def batch(b):
        code = sum(i * 16**j for j, i in enumerate(BATCHES[b]))
        count = len(BATCHES[b])
        used = pl.ds(0, count * pad)
        for i in BATCHES[b]:
            dispatch(b, (i // 4, i % 4))

        def weigh(j, t):
            i = lax.rem(lax.div(jnp.int32(code), t), 16)
            spot = lax.broadcasted_iota(jnp.int32, (cap, T), 0).astype(F32)
            for e in range(NE):
                hit = spot == slots[i, e : e + 1, :]
                weight = jnp.sum(
                    jnp.where(hit, slots[i, e + 4 : e + 5, :], 0.0), axis=1, keepdims=True
                )
                rows = pl.ds(pl.multiple_of(j * pad + e % 2 * (pad - cap), 8), cap)
                pv[e, rows, :] = jnp.broadcast_to(weight, (cap, 128))
            return t * 16

        lax.fori_loop(0, count, weigh, jnp.int32(1))

        def expert(e, _):
            gate_up = dot(xg[1, e, used, :], wgu[e])
            gate, up = gate_up[:, :FF], gate_up[:, FF:]
            hg = dot_nt(xg[0, e, used, :], wd[e])
            sigma = jax.nn.sigmoid(gate)
            active = gate * sigma
            hidden = (active * up).astype(BF).astype(F32)
            slot_prob = jnp.sum(hidden * hg, axis=1, keepdims=True)
            sp[e, used, :] = jnp.broadcast_to(slot_prob, (count * pad, 128))
            scaled = hg * pv[e, used, :][:, :1]
            gg = (scaled * up * sigma * (1.0 + gate * (1.0 - sigma))).astype(BF)
            ug = (scaled * active).astype(BF)
            xg[1, e, used, :] = dot_nt(jnp.concatenate([gg, ug], axis=1), wgu[e]).astype(BF)
            return 0

        lax.fori_loop(0, NE, expert, 0)

        def finish(j, t):
            i = lax.rem(lax.div(jnp.int32(code), t), 16)
            rows = pl.ds(pl.multiple_of(j * pad, pad), pad)
            cut = cap // 16 * 16
            for k in range(NE // 2):
                even, odd = xg[1, 2 * k, rows, :], xg[1, 2 * k + 1, rows, :]
                middle = jnp.concatenate(
                    [even[cut:].astype(F32)[:8], odd[:16].astype(F32)[8:]], axis=0
                ).astype(BF)
                o = 2 * cap * k
                srows[i, o : o + cut, :] = even[:cut]
                srows[i, o + cut : o + cut + 16, :] = middle
                srows[i, o + cut + 16 : o + 2 * cap, :] = odd[16:]
            spot = lax.broadcasted_iota(jnp.int32, (cap, T), 0).astype(F32)
            names = meta[i].astype(F32)[:8]
            out = jnp.zeros((8, T), F32)
            for e in range(NE):
                hit = spot == slots[i, e : e + 1, :]
                part = pl.ds(pl.multiple_of(j * pad + e % 2 * (pad - cap), 8), cap)
                val = jnp.sum(jnp.where(hit, sp[e, part, :][:, :1], 0.0), axis=0, keepdims=True)
                out = jnp.where(names == (ep * NE + e).astype(F32), val, out)
            ppg[i] = out.astype(BF)
            return t * 16

        lax.fori_loop(0, count, finish, jnp.int32(1))

    def leaf_up(v, l):
        return copy(
            ("up_leaf", v, l), srows.at[source(v, LEAF[l]), :, pl.ds(v * QD, QD)], fr.at[v, l],
            toward(v, LEAF[l], RAW[LEAF_PARENT[l]]),
        )

    def raw_up(v, k, c):
        rows = pl.ds(c * TC, TC)
        return copy(
            ("up_raw", v, k, c), pm.at[v, k - 1, rows], nm.at[v, k - 1, rows],
            toward(v, RAW[k], RAW[RAW_PARENT[k]]),
        )

    def return_leaf(*ls):
        for l in ls:
            for v in IMAGES:
                start(leaf_up(v, l))

    def children(k):
        return [l for l in range(NL) if LEAF_PARENT[l] == k], [c for c in range(1, len(RAW)) if RAW_PARENT[c] == k]

    def gathered(k, c, v, i, cols):
        leaves, raws = children(k)
        rows = pl.ds(c * TC, TC)
        lhs = jnp.concatenate([oh[i, :, rows]] + [oh[16 + 4 * l + v, :, rows] for l in leaves], axis=0)
        rhs = jnp.concatenate([srows[i, :, cols]] + [fr[v, l] for l in leaves], axis=0)
        res = dot_tn(lhs, rhs)
        for r in raws:
            res = res + nm[v, r - 1, rows, :].astype(F32)
        return res

    def wait_children(k, c, v):
        leaves, raws = children(k)
        if c == 0:
            for l in leaves:
                leaf_up(v, l).wait_recv()
        for r in raws:
            raw_up(v, r, c).wait_recv()

    def merge(k, c):
        for v in IMAGES:
            wait_children(k, c, v)

        def add(v, _):
            cols = pl.ds(pl.multiple_of(v * QD, QD), QD)
            pm[v, k - 1, pl.ds(c * TC, TC), :] = gathered(k, c, v, source_at(v, RAW[k]), cols).astype(BF)
            return 0

        lax.fori_loop(0, 4, add, 0)
        for v in IMAGES:
            start(raw_up(v, k, c))

    nodes = RAW[1:] + LEAF

    def pg_up(node):
        parent = parent_of(node)
        return copy(
            ("pg", node), ppg.at[source(0, node)], ppgr.at[nodes.index(node)], toward(0, node, parent)
        )

    def merge_pg(k):
        i = source(0, RAW[k])
        res = ppg[i].astype(F32)
        for node in nodes:
            if parent_of(node) == RAW[k]:
                pg_up(node).wait_recv()
                res = res + ppgr[nodes.index(node)].astype(F32)
        if k == 0:
            pg_out[...] = res
        else:
            ppg[i] = res.astype(BF)
            start(pg_up(RAW[k]))

    send_raw(1)
    wait_meta((0, 1), (1, 0))
    send_meta((0, 2), (1, 1), (3, 1), (2, 0), (1, 3))
    send_raw(2)
    clear()
    wait_meta((0, 3), (3, 0))
    prepare((0, 1, 3, 4, 12), range(0, 5))
    send_leaf(0, 1)
    weight_grads(0)
    wait_meta((0, 2), (2, 0))
    send_meta((1, 2), (3, 2), (2, 3), (2, 1))
    pass_raw(1, 3)
    pass_raw(2, 4)
    send_leaf(3)
    weight_grads(1)
    wait_meta((2, 3))
    send_meta((2, 2), (3, 3))
    for c in weights:
        c.wait()
    wait_leaf(0, 1)
    batch(0)
    wait_raw(3)
    pass_raw(4, 5)
    send_leaf(4, 2)
    wait_meta((1, 1), (3, 1), (1, 3), (1, 2), (3, 2), (2, 1))
    prepare((2, 8, 7, 13, 15, 6, 14, 9, 11), range(5, 10))
    wait_raw(5)
    send_leaf(8, 9)
    send_leaf(5, 6, 7)
    wait_leaf(3, 4)
    batch(1)
    return_leaf(3, 4)
    weight_grads(2)
    wait_meta((2, 2), (3, 3))
    prepare((5, 10), ())
    wait_leaf(2, 8, 9)
    batch(2)
    return_leaf(8, 9, 2)
    weight_grads(3)
    wait_leaf(5, 6, 7)
    batch(3)
    return_leaf(5, 6)
    for node in LEAF:
        start(pg_up(node))
    merge(5, 0)
    merge(5, 1)
    return_leaf(7)
    merge_pg(5)
    merge(3, 0)
    merge(3, 1)
    merge_pg(3)
    return_leaf(0, 1)
    merge(4, 0)
    merge(1, 0)
    merge(4, 1)
    merge_pg(4)
    merge_pg(1)
    merge(2, 0)
    merge(1, 1)
    merge_pg(2)
    merge(2, 1)
    ups = {}
    for c in range(CHUNKS):
        for v in IMAGES:
            rows, cols = pl.ds(c * TC, TC), pl.ds(v * QD, QD)
            wait_children(0, c, v)
            upv[rows, cols] = gathered(0, c, v, 0, cols).astype(BF)
            ups[v, c] = copy(("up", v, c), upv.at[rows, cols], up_out.at[rows, cols], before)

            @pl.when(sec > 0)
            def _():
                ups[v, c].start()

    merge_pg(0)

    for c in sent:
        c.wait_send()
    for c in ups.values():
        @pl.when(sec > 0)
        def _():
            c.wait_send()

        @pl.when(sec < sections - 1)
        def _():
            c.wait_recv()


def deliver(up_in, pg_in, go_in, uo_in, up_out, pg_out, go_out, uo_out, sem):
    out = [(up_in, up_out)]
    for e in range(go_in.shape[0]):
        out += [(go_in.at[e], go_out.at[e]), (uo_in.at[e], uo_out.at[e])]
    out = [pltpu.make_async_copy(v, o, sem.at[k]) for k, (v, o) in enumerate(out)]
    for c in out:
        c.start()
    pg_out[...] = pg_in[...].astype(BF)
    for c in out:
        c.wait()


def per_device(sections, og, li, ids, probs, wg, wu, wd, si, sg, su, counts):
    T, D = og.shape[1], og.shape[2]
    NE, FF = wg.shape[1], wg.shape[3]
    SL = si.shape[2]
    cap = SL // 16
    pad = -(-cap // 16) * 16
    M, R = NE * cap, max(map(len, BATCHES)) * pad
    HD, QD = D // 2, D // 4
    hbm = pl.BlockSpec(memory_space=pl.ANY)
    V = pltpu.VMEM
    up, pg, go, uo = pl.pallas_call(
        functools.partial(kernel, sections, cap, pad),
        out_shape=(
            V((T, D), BF),
            V((8, T), F32),
            V((NE, D, FF), BF),
            V((NE, D, FF), BF),
        ),
        in_specs=[hbm] * 2 + [pl.BlockSpec(memory_space=V)] * 2 + [hbm] * 6 + [pl.BlockSpec(memory_space=pltpu.SMEM)],
        out_specs=(pl.BlockSpec(memory_space=V),) * 4,
        scratch_shapes=[
            V((4, len(RAW), T, HD), BF), V((4, NL, M, HD), BF), V((4, NL, M, HD), BF),
            V((16, 16, T), BF), V((NE, D, 2 * FF), BF), V((NE, FF, D), BF),
            V((SL, D), BF), V((2, SL, FF), BF), V((SL, 2 * FF), BF),
            V((PAIRS, 8, T), F32), V((PAIRS, 8, T), F32), V((T, T), BF), V((PAIRS, M, T), BF),
            V((2, NE, R, D), BF), V((NE, R, 128), F32), V((NE, R, 128), F32), V((16, M, D), BF),
            V((4, NL, M, QD), BF), V((4, len(RAW) - 1, T, QD), BF), V((4, len(RAW) - 1, T, QD), BF),
            V((T, D), BF), V((16, 8, T), BF), V((16, 8, T), BF),
            pltpu.SemaphoreType.DMA((N_SEMS,)), pltpu.SemaphoreType.DMA((N_SEMS,)),
            pltpu.SemaphoreType.DMA((14,)),
        ],
        compiler_params=pltpu.CompilerParams(
            collective_id=0, has_side_effects=True, vmem_limit_bytes=60_150_000
        ),
    )(og[0], li[0], ids[0].T, probs[0].T, wg[0], wu[0], wd[0], si[0], sg[0], su[0], counts[0])
    up, pg, go, uo = pl.pallas_call(
        deliver,
        out_shape=(
            jax.ShapeDtypeStruct((T, D), BF),
            jax.ShapeDtypeStruct((8, T), BF),
            jax.ShapeDtypeStruct((NE, D, FF), BF),
            jax.ShapeDtypeStruct((NE, D, FF), BF),
        ),
        in_specs=[pl.BlockSpec(memory_space=V)] * 4,
        out_specs=(hbm, pl.BlockSpec(memory_space=V), hbm, hbm),
        scratch_shapes=[pltpu.SemaphoreType.DMA((1 + 2 * NE,))],
        compiler_params=pltpu.CompilerParams(vmem_limit_bytes=16 * 2**20),
    )(up, pg, go, uo)
    return up[None], pg.T[None], go[None], uo[None]


def solution(mesh):
    return jax.shard_map(
        functools.partial(per_device, mesh.shape["section"]),
        mesh=mesh,
        in_specs=(
            P("section", "ep", None),
            P("section", "ep", None),
            P("section", "ep", None),
            P("section", "ep", None),
            P("section", "ep", None, None),
            P("section", "ep", None, None),
            P("section", "ep", None, None),
            P("section", "ep", None, None),
            P("section", "ep", None, None),
            P("section", "ep", None, None),
            P("section", "ep", None),
        ),
        out_specs=(
            P("section", "ep", None),
            P("section", "ep", None),
            P("section", "ep", None, None),
            P("section", "ep", None, None),
        ),
        check_vma=False,
    )
```
